16 devices in a mesh: batch: 2 (over y, z), seq: 8 (over x, core).
Axes of the slice: x: 4, y: 2, z: 1, core: 2. Of those that a mesh axis runs over, the one named last changes fastest.
The devices are a block of a 4x4x8 slice.
Arguments:
- msa_act: bfloat16 [1024, 384, 64], P(('batch', 'seq')), parts along dimension 0
- msa_mask: int32 [1024, 384], P(('batch', 'seq')), parts along dimension 0
- pair_act: bfloat16 [768, 384, 128], P(('batch', 'seq')), parts along dimension 0
- w_pair_bias: bfloat16 [128, 8], replicated
- w_row_in: bfloat16 [64, 256], replicated
- b_row_gate: bfloat16 [64], replicated
- w_row_out: bfloat16 [64, 64], replicated
- w_col_in: bfloat16 [64, 144], replicated
- b_col_gate: bfloat16 [64], replicated
- w_col_out: bfloat16 [64, 64], replicated
- w_trans_in: bfloat16 [64, 256], replicated
- w_trans_out: bfloat16 [256, 64], replicated
- w_opm_in: bfloat16 [64, 64], replicated
- w_opm_out: bfloat16 [32, 32, 128], replicated
- b_opm_out: bfloat16 [128], replicated
Outputs:
- output 1: bfloat16 [1024, 384, 64], P(('batch', 'seq')), parts along dimension 0
- output 2: bfloat16 [768, 384, 128], P(('batch', 'seq')), parts along dimension 0
There are 2 independent parts. The reference program is written for one: setup_inputs(seed, part) draws one part's arguments, and reference() takes and returns one part's arrays. A program takes and returns all parts, laid end to end along the dimension named above; an argument that names none is the same for every part.
All inputs are finite; a program needn't handle non-finite values.
Results may differ from the reference program's by a relative error of at most 0.0113807.
Values are sent between devices in bfloat16 or wider.
A program may use at most 768 MiB of HBM per device.

```python
import jax
import jax.numpy as jnp
from jax import lax

NUM_SEQ = 512
NUM_RES = 384
MSA_DIM = 64
PAIR_DIM = 128
NUM_HEADS = 8
HEAD_DIM = 8
OPM_DIM = 32


def layer_norm(values):
    as_float = values.astype(jnp.float32)
    centered = as_float - jnp.mean(as_float, axis=-1, keepdims=True)
    variance = jnp.mean(centered * centered, axis=-1, keepdims=True)
    return (centered * lax.rsqrt(variance + 1e-5)).astype(jnp.bfloat16)


def project(values, weight):
    lead_shape = values.shape[:-1]
    flat_rows = values.reshape(-1, values.shape[-1])
    return jnp.dot(flat_rows, weight, preferred_element_type=jnp.float32).reshape(lead_shape + (weight.shape[1],))


def draw_mask(mask_key):
    key_set = jax.random.split(mask_key, 3)
    n_valid = jax.random.randint(key_set[0], (), NUM_SEQ // 2, NUM_SEQ + 1)
    starts = jax.random.randint(key_set[1], (NUM_SEQ, 1), 0, NUM_RES // 4)
    lengths = jax.random.randint(key_set[2], (NUM_SEQ, 1), NUM_RES // 2, NUM_RES + 1)
    residue = jnp.arange(NUM_RES)[None, :]
    seq_index = jnp.arange(NUM_SEQ)[:, None]
    covered = (residue >= starts) & (residue < starts + lengths) & (seq_index < n_valid)
    return (covered | (seq_index == 0)).astype(jnp.int32)


def normal_weight(weight_key, weight_shape, factor):
    return (jax.random.normal(weight_key, weight_shape, jnp.float32) * factor).astype(jnp.bfloat16)


def setup_inputs(seed: int = 0, part: int = 0) -> dict:
    part_key = jax.random.fold_in(jax.random.key(seed), part)
    data_keys = jax.random.split(part_key, 5)
    weight_keys = jax.random.split(jax.random.key(seed + 1), 12)
    head_total = NUM_HEADS * HEAD_DIM
    seq_depth = jnp.linspace(-1.5, 1.5, NUM_SEQ, dtype=jnp.float32)
    base_rows = jax.random.normal(data_keys[0], (NUM_RES, MSA_DIM), jnp.float32)
    direction = jax.random.normal(data_keys[1], (NUM_RES, MSA_DIM), jnp.float32)
    msa_noise = jax.random.normal(data_keys[2], (NUM_SEQ, NUM_RES, MSA_DIM), jnp.float32)
    msa_act = base_rows[None] + seq_depth[:, None, None] * direction[None] + 0.8 * msa_noise
    pair_act = jax.random.normal(data_keys[4], (NUM_RES, NUM_RES, PAIR_DIM), jnp.float32)
    return {
        'msa_act': msa_act.astype(jnp.bfloat16),
        'msa_mask': draw_mask(data_keys[3]),
        'pair_act': pair_act.astype(jnp.bfloat16),
        'w_pair_bias': normal_weight(weight_keys[0], (PAIR_DIM, NUM_HEADS), 1.5 * PAIR_DIM ** -0.5),
        'w_row_in': normal_weight(weight_keys[1], (MSA_DIM, 4 * head_total), MSA_DIM ** -0.5),
        'b_row_gate': normal_weight(weight_keys[2], (head_total,), 1.0),
        'w_row_out': normal_weight(weight_keys[3], (head_total, MSA_DIM), 3.0 * head_total ** -0.5),
        'w_col_in': normal_weight(weight_keys[4], (MSA_DIM, 2 * head_total + 2 * HEAD_DIM), MSA_DIM ** -0.5),
        'b_col_gate': normal_weight(weight_keys[5], (head_total,), 1.0),
        'w_col_out': normal_weight(weight_keys[6], (head_total, MSA_DIM), 2.0 * head_total ** -0.5),
        'w_trans_in': normal_weight(weight_keys[7], (MSA_DIM, 4 * MSA_DIM), MSA_DIM ** -0.5),
        'w_trans_out': normal_weight(weight_keys[8], (4 * MSA_DIM, MSA_DIM), 1.5 * (4 * MSA_DIM) ** -0.5),
        'w_opm_in': normal_weight(weight_keys[9], (MSA_DIM, 2 * OPM_DIM), MSA_DIM ** -0.5),
        'w_opm_out': normal_weight(weight_keys[10], (OPM_DIM, OPM_DIM, PAIR_DIM), 2.0 / OPM_DIM),
        'b_opm_out': normal_weight(weight_keys[11], (PAIR_DIM,), 0.5),
    }


def reference(msa_act, msa_mask, pair_act, w_pair_bias, w_row_in, b_row_gate, w_row_out, w_col_in, b_col_gate, w_col_out, w_trans_in, w_trans_out, w_opm_in, w_opm_out, b_opm_out):
    head_total = NUM_HEADS * HEAD_DIM
    attn_scale = HEAD_DIM ** -0.5
    seq_blk = 4
    row_blk = 16
    keep_mask = msa_mask > 0
    mask_float = msa_mask.astype(jnp.float32)

    pair_bias = project(layer_norm(pair_act), w_pair_bias).astype(jnp.bfloat16)
    bias_heads = jnp.transpose(pair_bias, (2, 0, 1)).astype(jnp.float32)
    row_proj = project(layer_norm(msa_act), w_row_in).astype(jnp.bfloat16)
    row_proj = row_proj.reshape(NUM_SEQ // seq_blk, seq_blk, NUM_RES, 4, NUM_HEADS, HEAD_DIM)
    gate_bias = b_row_gate.astype(jnp.float32).reshape(NUM_HEADS, HEAD_DIM)

    def row_block(block_in):
        proj_blk, keep_blk = block_in
        q_blk = proj_blk[:, :, 0].astype(jnp.float32)
        k_blk = proj_blk[:, :, 1].astype(jnp.float32)
        v_blk = proj_blk[:, :, 2].astype(jnp.float32)
        g_blk = proj_blk[:, :, 3].astype(jnp.float32)
        scores = jnp.einsum('sihd,sjhd->shij', q_blk, k_blk) * attn_scale + bias_heads[None]
        scores = jnp.where(keep_blk[:, None, None, :], scores, -1e9)
        attn_probs = jax.nn.softmax(scores, axis=-1).astype(jnp.bfloat16).astype(jnp.float32)
        attended = jnp.einsum('shij,sjhd->sihd', attn_probs, v_blk)
        return (jax.nn.sigmoid(g_blk + gate_bias) * attended).astype(jnp.bfloat16)

    gated_row = lax.map(row_block, (row_proj, keep_mask.reshape(NUM_SEQ // seq_blk, seq_blk, NUM_RES)))
    gated_row = gated_row.reshape(NUM_SEQ, NUM_RES, head_total)
    msa_one = (msa_act.astype(jnp.float32) + project(gated_row, w_row_out)).astype(jnp.bfloat16)

    col_proj = project(layer_norm(msa_one), w_col_in).astype(jnp.bfloat16)
    q_col = col_proj[:, :, :head_total].reshape(NUM_SEQ, NUM_RES, NUM_HEADS, HEAD_DIM).astype(jnp.float32)
    g_col = col_proj[:, :, head_total:2 * head_total].astype(jnp.float32)
    k_col = col_proj[:, :, 2 * head_total:2 * head_total + HEAD_DIM].astype(jnp.float32)
    v_col = col_proj[:, :, 2 * head_total + HEAD_DIM:].astype(jnp.float32)
    q_sum = jnp.einsum('si,sihd->ihd', mask_float, q_col)
    counts = jnp.sum(mask_float, axis=0)
    q_bar = (q_sum / (counts[:, None, None] + 1e-10)).astype(jnp.bfloat16).astype(jnp.float32)
    logits = jnp.einsum('ihd,sid->sih', q_bar, k_col) * attn_scale
    logits = jnp.where(keep_mask[:, :, None], logits, -1e9)
    col_probs = jax.nn.softmax(logits, axis=0)
    col_out = jnp.einsum('sih,sid->ihd', col_probs, v_col).reshape(NUM_RES, head_total)
    col_gate = jax.nn.sigmoid(g_col + b_col_gate.astype(jnp.float32))
    gated_col = (col_gate * col_out[None]).astype(jnp.bfloat16)
    msa_two = (msa_one.astype(jnp.float32) + project(gated_col, w_col_out)).astype(jnp.bfloat16)

    hidden = jnp.maximum(project(layer_norm(msa_two), w_trans_in), 0.0).astype(jnp.bfloat16)
    msa_three = (msa_two.astype(jnp.float32) + project(hidden, w_trans_out)).astype(jnp.bfloat16)

    opm_proj = (project(layer_norm(msa_three), w_opm_in).astype(jnp.bfloat16) * msa_mask[:, :, None].astype(jnp.bfloat16)).astype(jnp.float32)
    left_vec = opm_proj[:, :, :OPM_DIM]
    right_vec = opm_proj[:, :, OPM_DIM:]
    norm_pair = jnp.dot(mask_float.T, mask_float, preferred_element_type=jnp.float32)
    w_opm_float = w_opm_out.astype(jnp.float32)
    left_blocks = jnp.moveaxis(left_vec.reshape(NUM_SEQ, NUM_RES // row_blk, row_blk, OPM_DIM), 1, 0)
    norm_blocks = norm_pair.reshape(NUM_RES // row_blk, row_blk, NUM_RES)

    def outer_block(block_in):
        left_blk, norm_blk = block_in
        outer_sum = jnp.einsum('sic,sjd->ijcd', left_blk, right_vec)
        mean_outer = outer_sum / (norm_blk[:, :, None, None] + 1e-3)
        return jnp.einsum('ijcd,cde->ije', mean_outer, w_opm_float)

    pair_update = lax.map(outer_block, (left_blocks, norm_blocks)).reshape(NUM_RES, NUM_RES, PAIR_DIM)
    pair_out = (pair_act.astype(jnp.float32) + pair_update + b_opm_out.astype(jnp.float32)).astype(jnp.bfloat16)
    return msa_three, pair_out
```

```python
import functools
import math

import jax
import jax.numpy as jnp
from jax import lax
from jax.experimental import pallas as pl
from jax.experimental.pallas import tpu as pltpu
from jax.sharding import PartitionSpec as P

MASK_FILL = -1e9
LOG2E = math.log2(math.e)
F32 = jnp.float32
BF16 = jnp.bfloat16
VMEM_LIMIT = 62 * 1024 * 1024
MESH = pl.DeviceIdType.MESH
SEQS = 4


def layer_norm(values):
    as_float = values.astype(F32)
    centered = as_float - jnp.mean(as_float, axis=-1, keepdims=True)
    variance = jnp.mean(centered * centered, axis=-1, keepdims=True)
    return (centered * lax.rsqrt(variance + 1e-5)).astype(BF16)


def norm_rows(x):
    c = x - jnp.mean(x, axis=0, keepdims=True)
    var = jnp.mean(c * c, axis=0, keepdims=True)
    return (c * lax.rsqrt(var + 1e-5)).astype(BF16)


def dot(a, b):
    return jnp.dot(a, b, preferred_element_type=F32)


def dot_t(a, b):
    return lax.dot_general(a, b, (((1,), (1,)), ((), ())), preferred_element_type=F32)


def sigmoid(x):
    return 1.0 / (1.0 + jnp.exp(-x))


def wide_max(x):
    return jnp.max(jnp.max(x, axis=0, keepdims=True), axis=1, keepdims=True)[0, 0]


def row_kernel(heads, hd, scale, e_ref, m_ref, bias_ref, win_ref, bg_ref, wout_ref, cin_ref,
               e1_ref, g_ref, kv_ref, qsum_ref, rhs_ref, kaug_ref, va_ref, att_ref, top_ref):
    us, res, ch = e_ref.shape
    ht = heads * hd
    wide = us * res
    step = pl.program_id(0)

    @pl.when(step == 0)
    def _():
        rows = lax.broadcasted_iota(jnp.int32, rhs_ref.shape, 1)
        rhs_ref[...] = jnp.where(rows == 2 * ht, 1.0, 0.0).astype(BF16)
        qsum_ref[...] = jnp.zeros_like(qsum_ref)
        top = jnp.abs(bias_ref[0])
        for pr in range(1, heads // 2):
            top = jnp.maximum(top, jnp.abs(bias_ref[pr]))
        top_ref[0] = wide_max(top)

    eye = (lax.broadcasted_iota(jnp.int32, (ch, ch), 0) == lax.broadcasted_iota(jnp.int32, (ch, ch), 1)).astype(BF16)
    x = dot_t(eye, e_ref[...].reshape(wide, ch))
    proj = dot(win_ref[...], norm_rows(x)).astype(BF16).astype(F32)
    q, k, v, g = (proj[n * ht:(n + 1) * ht] for n in range(4))
    keep = m_ref[0]
    qs = q * (scale * LOG2E)
    q_top = wide_max(jnp.sum((qs * qs).reshape(heads, hd, wide), axis=1))
    k_top = wide_max(jnp.sum((k * k).reshape(heads, hd, wide), axis=1))
    small = (q_top * k_top < 900.0) & (top_ref[0] < 30.0)

    first_half = (lax.broadcasted_iota(jnp.int32, (ht, wide), 0) % 16) < 8
    hi = qs.astype(BF16).astype(F32)
    for n, part in enumerate((hi, qs - hi)):
        even = jnp.where(first_half, part, 0.0).astype(BF16)
        odd = jnp.where(first_half, 0.0, part).astype(BF16)
        for u in range(us):
            for h in range(heads):
                rows = slice(16 * (h // 2), 16 * (h // 2) + 16)
                rhs_ref[u, n * ht + rows.start:n * ht + rows.stop, h * res:(h + 1) * res] = \
                    (odd if h % 2 else even)[rows, u * res:(u + 1) * res]
    pen = jnp.where(lax.broadcasted_iota(jnp.int32, (16, wide), 0) == 0,
                    jnp.broadcast_to(jnp.where(keep > 0, 0.0, -1e30), (16, wide)), 0.0)
    kaug_ref[...] = jnp.transpose(jnp.concatenate([k, k, pen], axis=0)).astype(BF16)
    ones = jnp.where(lax.broadcasted_iota(jnp.int32, (8, wide), 0) == 0, 1.0, 0.0)
    for pr in range(heads // 2):
        va_ref[pr] = jnp.concatenate([v[16 * pr:16 * pr + 8], ones, v[16 * pr + 8:16 * pr + 16], ones], axis=0).astype(BF16)

    @pl.when(small)
    def _():
        for u in range(us):
            cols = slice(u * res, (u + 1) * res)
            for pr in range(heads // 2):
                s = dot(kaug_ref[cols], rhs_ref[u, :, 2 * pr * res:(2 * pr + 2) * res]) + bias_ref[pr]
                o = dot(va_ref[pr, :, cols], jnp.exp2(s).astype(BF16))
                att_ref[16 * pr:16 * pr + 8, cols] = o[0:8, :res] / o[8:9, :res]
                att_ref[16 * pr + 8:16 * pr + 16, cols] = o[16:24, res:] / o[24:25, res:]
            some = jnp.max(keep[:, cols], axis=1, keepdims=True) > 0
            flat = jnp.mean(v[:, cols], axis=1, keepdims=True)
            att_ref[:, cols] = jnp.where(some, att_ref[:, cols], flat)

    @pl.when(jnp.logical_not(small))
    def _():
        def one(t, _):
            u, pr = t // (heads // 2), t % (heads // 2)
            cols = pl.ds(pl.multiple_of(u * res, res), res)
            s = dot(kaug_ref[cols], rhs_ref[u, :, pl.ds(pl.multiple_of(2 * pr * res, 2 * res), 2 * res)]) + bias_ref[pr]
            p = jnp.exp2(s - jnp.max(s, axis=0, keepdims=True)).astype(BF16)
            o = dot(va_ref[pr, :, cols], p)
            att_ref[pl.ds(pl.multiple_of(16 * pr, 16), 8), cols] = o[0:8, :res] / o[8:9, :res]
            att_ref[pl.ds(pl.multiple_of(16 * pr + 8, 8), 8), cols] = o[16:24, res:] / o[24:25, res:]
            return 0

        lax.fori_loop(0, us * (heads // 2), one, 0)

    gated = (sigmoid(g + bg_ref[...]) * att_ref[...]).astype(BF16)
    e1 = (x + dot(wout_ref[...], gated)).astype(BF16)
    e1_ref[0] = e1
    col = dot(cin_ref[...], norm_rows(e1.astype(F32))).astype(BF16)
    part = col[:ht].astype(F32) * keep
    tot = part[:, :res]
    for u in range(1, us):
        tot = tot + part[:, u * res:(u + 1) * res]
    qsum_ref[...] += tot
    g_ref[0] = col[ht:2 * ht]
    kv_ref[0] = col[2 * ht:]


def exchange(axis, me, n, srcs, dst, send_sem, recv_sem):
    copies = []
    for t in range(1, n):
        peer = lax.rem(me + t, n)
        copy = pltpu.make_async_remote_copy(src_ref=srcs(peer), dst_ref=dst.at[me], send_sem=send_sem.at[t],
                                            recv_sem=recv_sem.at[t], device_id={axis: peer}, device_id_type=MESH)
        copy.start()
        copies.append(copy)
    return copies


def col_kernel(axis, n, heads, hd, scale, qsum_ref, cnt_ref, kv_ref, m_ref, o_ref,
               l_ref, qp_ref, qb_ref, st_ref, sp_ref, send_sem, recv_sem):
    ng, _, wide = kv_ref.shape
    res = qsum_ref.shape[1]
    us = wide // res
    ht = heads * hd
    me = lax.axis_index(axis)
    barrier = pltpu.get_barrier_semaphore()
    for t in range(1, n):
        pl.semaphore_signal(barrier, inc=1, device_id={axis: lax.rem(me + t, n)}, device_id_type=MESH)
    pl.semaphore_wait(barrier, n - 1)

    blk = ht // n
    mine = pl.ds(pl.multiple_of(me * blk, blk), blk)
    copies = exchange(axis, me, n, lambda p: qsum_ref.at[pl.ds(pl.multiple_of(p * blk, blk), blk)], qp_ref,
                      send_sem.at[0], recv_sem.at[0])
    qp_ref[me] = qsum_ref[mine]
    for c in copies:
        c.wait()
    tot = qp_ref[0]
    for t in range(1, n):
        tot = tot + qp_ref[t]
    qb_ref[me] = (tot / (cnt_ref[...] + 1e-10)).astype(BF16).astype(F32)
    copies = exchange(axis, me, n, lambda p: qb_ref.at[me], qb_ref, send_sem.at[1], recv_sem.at[1])
    for c in copies:
        c.wait()
    qbar = qb_ref[...].reshape(ht, res)

    def logits(gr, top):
        for u in range(us):
            cols = slice(u * res, (u + 1) * res)
            kv = kv_ref[gr, :, cols].astype(F32)
            acc = qbar[0:heads] * kv[0:1]
            for d in range(1, hd):
                acc = acc + qbar[d * heads:(d + 1) * heads] * kv[d:d + 1]
            acc = jnp.where(m_ref[gr, :, cols] > 0, acc * scale, MASK_FILL)
            l_ref[gr, :, cols] = acc
            top = jnp.maximum(top, acc)
        return top

    top = lax.fori_loop(0, ng, logits, jnp.full((heads, res), -3e38, F32))

    def sums(gr, carry):
        for u in range(us):
            cols = slice(u * res, (u + 1) * res)
            w = jnp.exp(l_ref[gr, :, cols] - top)
            kv = kv_ref[gr, :, cols].astype(F32)
            carry = (carry[0] + w,) + tuple(carry[1 + d] + w * kv[hd + d:hd + d + 1] for d in range(hd))
        return carry

    zero = jnp.zeros((heads, res), F32)
    tot = lax.fori_loop(0, ng, sums, (zero,) * (hd + 1))
    for d in range(hd):
        st_ref[:, d, :] = tot[1 + d]
    st_ref[:, hd, :] = tot[0]
    st_ref[:, hd + 1, :] = top
    for d in range(hd + 2, st_ref.shape[1]):
        st_ref[:, d, :] = zero
    copies = exchange(axis, me, n, lambda p: st_ref.at[p], sp_ref, send_sem.at[2], recv_sem.at[2])
    sp_ref[me] = st_ref[me]
    for c in copies:
        c.wait()
    best = sp_ref[0, hd + 1:hd + 2]
    for t in range(1, n):
        best = jnp.maximum(best, sp_ref[t, hd + 1:hd + 2])
    num = jnp.zeros((hd, res), F32)
    den = jnp.zeros((1, res), F32)
    for t in range(n):
        fac = jnp.exp(sp_ref[t, hd + 1:hd + 2] - best)
        num = num + sp_ref[t, 0:hd] * fac
        den = den + sp_ref[t, hd:hd + 1] * fac
    o_ref[me] = num / den
    copies = exchange(axis, me, n, lambda p: o_ref.at[me], o_ref, send_sem.at[3], recv_sem.at[3])
    for c in copies:
        c.wait()


def tail_kernel(o_ref, e1_ref, g_ref, m_ref, bg_ref, wout_ref, tin_ref, tout_ref, opm_ref, e3_ref, ab_ref, buf_ref):
    ht, res = o_ref.shape
    us = e1_ref.shape[2] // res
    blk = 128
    eye = (lax.broadcasted_iota(jnp.int32, (blk, blk), 0) == lax.broadcasted_iota(jnp.int32, (blk, blk), 1)).astype(BF16)
    o = jnp.concatenate([o_ref[...]] * us, axis=1)
    for gr in range(e1_ref.shape[0]):
        gated = (sigmoid(g_ref[gr].astype(F32) + bg_ref[...]) * o).astype(BF16)
        e2 = (e1_ref[gr].astype(F32) + dot(wout_ref[...], gated)).astype(BF16).astype(F32)
        hid = jnp.maximum(dot(tin_ref[...], norm_rows(e2)), 0.0).astype(BF16)
        e3 = (e2 + dot(tout_ref[...], hid)).astype(BF16)
        ab = dot(opm_ref[...], norm_rows(e3.astype(F32))).astype(BF16).astype(F32) * m_ref[gr]
        for u in range(us):
            for t in range(res // blk):
                at = u * res + t * blk
                e3_ref[gr * us + u, t * blk:(t + 1) * blk, :] = dot_t(eye, e3[:, at:at + blk]).astype(BF16)
            buf_ref[:, gr * us + u, :] = ab[:, u * res:(u + 1) * res]
    ab_ref[...] = buf_ref[...].astype(BF16)


def opm_kernel(odim, a_ref, b_ref, z_ref, ninv_ref, w_ref, bo_ref, out_ref, hi_ref, lo_ref):
    ndev, _, ns, jb = b_ref.shape
    ib = z_ref.shape[0]
    a = a_ref[...]
    for q in range(odim // 2):
        rhs = jnp.concatenate([b_ref[:, 2 * q].reshape(ndev * ns, jb), b_ref[:, 2 * q + 1].reshape(ndev * ns, jb)], axis=1)
        pr = dot(a, rhs)
        hi = pr.astype(BF16)
        lo = (pr - hi.astype(F32)).astype(BF16)
        for val, ref in ((hi, hi_ref), (lo, lo_ref)):
            for i in range(ib):
                for t in range(2):
                    ref[i // 2, (2 * q + t) * odim:(2 * q + t + 1) * odim, (i % 2) * jb:(i % 2 + 1) * jb] = \
                        val[i * odim:(i + 1) * odim, t * jb:(t + 1) * jb]
    for ip in range(ib // 2):
        zt = dot(w_ref[...], hi_ref[ip]) + dot(w_ref[...], lo_ref[ip])
        for t in range(2):
            i = 2 * ip + t
            upd = jnp.transpose(zt[:, t * jb:(t + 1) * jb] * ninv_ref[i])
            out_ref[i] = (z_ref[i].astype(F32) + upd + bo_ref[...]).astype(BF16)


def solution(mesh):
    row_spec = P(('batch', 'seq'))
    rep_spec = P()
    n_seq = mesh.shape['seq']

    def local_block(msa, mask, pair, w_pair_bias, w_row_in, b_row_gate, w_row_out, w_col_in, b_col_gate, w_col_out,
                    w_trans_in, w_trans_out, w_opm_in, w_opm_out, b_opm_out):
        ns, res, ch = msa.shape
        rows = pair.shape[0]
        pd = pair.shape[-1]
        heads = w_pair_bias.shape[1]
        ht = w_row_out.shape[0]
        hd = ht // heads
        odim = w_opm_out.shape[0]
        scale = hd ** -0.5
        params = functools.partial(pltpu.CompilerParams, vmem_limit_bytes=VMEM_LIMIT)

        bias_rows = jnp.einsum('ijc,ch->hij', layer_norm(pair), w_pair_bias, preferred_element_type=F32).astype(BF16)
        packed = jnp.concatenate([bias_rows.reshape(heads * rows, res), mask.astype(BF16)], axis=0)
        packed = lax.all_gather(packed, 'seq', axis=0)
        bias_all = packed[:, :heads * rows].reshape(n_seq, heads, rows, res)
        bias_t = jnp.transpose(bias_all, (1, 3, 0, 2)).reshape(heads // 2, 2, res, res)
        bias_t = jnp.transpose(bias_t, (0, 2, 1, 3)).reshape(heads // 2, res, 2 * res).astype(F32) * LOG2E
        mask_all = packed[:, heads * rows:].reshape(n_seq * ns, res)
        counts = jnp.sum(mask_all.astype(F32), axis=0, keepdims=True)
        me = lax.axis_index('seq')
        mask_mine = lax.dynamic_slice_in_dim(mask_all, me * rows, rows, axis=1)
        ninv = 1.0 / (jnp.einsum('si,sj->ij', mask_mine, mask_all, preferred_element_type=F32) + 1e-3)

        us = SEQS
        ng, wide = ns // us, us * res
        mask_f = mask.astype(F32).reshape(ng, 1, wide)
        perm_q = w_col_in[:, :ht].reshape(ch, heads, hd).transpose(0, 2, 1).reshape(ch, ht)
        cin = jnp.concatenate([perm_q, w_col_in[:, ht:]], axis=1).T
        ncol = cin.shape[0]
        bcg = b_col_gate.reshape(ht, 1).astype(F32)
        brg = b_row_gate.reshape(ht, 1).astype(F32)

        full = lambda *shape: pl.BlockSpec(shape, lambda *g: (0,) * len(shape))
        group = lambda k, r: pl.BlockSpec((k, r, wide), lambda s: (s, 0, 0))
        e1, gate, kv, qsum = pl.pallas_call(
            functools.partial(row_kernel, heads, hd, scale),
            grid=(ng,),
            in_specs=[pl.BlockSpec((us, res, ch), lambda s: (s, 0, 0)), group(1, 1),
                      full(heads // 2, res, 2 * res), full(4 * ht, ch), full(ht, 1), full(ch, ht), full(ncol, ch)],
            out_specs=[group(1, ch), group(1, ht), group(1, 2 * hd), full(ht, res)],
            out_shape=[jax.ShapeDtypeStruct((ng, ch, wide), BF16), jax.ShapeDtypeStruct((ng, ht, wide), BF16),
                       jax.ShapeDtypeStruct((ng, 2 * hd, wide), BF16), jax.ShapeDtypeStruct((ht, res), F32)],
            scratch_shapes=[pltpu.VMEM((us, 2 * ht + 16, heads * res), BF16), pltpu.VMEM((wide, 2 * ht + 16), BF16),
                            pltpu.VMEM((heads // 2, 32, wide), BF16), pltpu.VMEM((ht, wide), F32), pltpu.SMEM((1,), F32)],
            compiler_params=params(dimension_semantics=('arbitrary',)),
            name='row_attention',
        )(msa, mask_f, bias_t, w_row_in.T, brg, w_row_out.T, cin)

        col_o = pl.pallas_call(
            functools.partial(col_kernel, 'seq', n_seq, heads, hd, scale),
            in_specs=[pl.BlockSpec(memory_space=pltpu.VMEM)] * 4,
            out_specs=pl.BlockSpec(memory_space=pltpu.VMEM),
            out_shape=jax.ShapeDtypeStruct((heads, hd, res), F32),
            scratch_shapes=[pltpu.VMEM((ng, heads, wide), F32), pltpu.VMEM((n_seq, ht // n_seq, res), F32),
                            pltpu.VMEM((n_seq, ht // n_seq, res), F32), pltpu.VMEM((heads, 16, res), F32),
                            pltpu.VMEM((n_seq, 16, res), F32), pltpu.SemaphoreType.DMA((4, n_seq)),
                            pltpu.SemaphoreType.DMA((4, n_seq))],
            compiler_params=params(collective_id=0, has_side_effects=True),
            name='col_stats',
        )(qsum, counts, kv, mask_f).reshape(ht, res)

        tb = 16
        e3, ab = pl.pallas_call(
            tail_kernel,
            grid=(ns // tb,),
            in_specs=[full(ht, res), group(tb // us, ch), group(tb // us, ht), group(tb // us, 1),
                      full(ht, 1), full(ch, ht), full(w_trans_in.shape[1], ch), full(ch, w_trans_in.shape[1]),
                      full(2 * odim, ch)],
            out_specs=[pl.BlockSpec((tb, res, ch), lambda s: (s, 0, 0)), pl.BlockSpec((2 * odim, tb, res), lambda s: (0, s, 0))],
            out_shape=[jax.ShapeDtypeStruct((ns, res, ch), BF16), jax.ShapeDtypeStruct((2 * odim, ns, res), BF16)],
            scratch_shapes=[pltpu.VMEM((2 * odim, tb, res), F32)],
            compiler_params=params(dimension_semantics=('arbitrary',)),
            name='tail',
        )(col_o, e1, gate, mask_f, bcg, w_col_out.T, w_trans_in.T, w_trans_out.T, w_opm_in.T)

        b_all = lax.all_gather(ab[odim:], 'seq', axis=0)
        a_own = lax.all_to_all(ab[:odim].reshape(odim, ns, n_seq, rows), 'seq', split_axis=2, concat_axis=0)
        a_own = a_own.reshape(n_seq, odim, ns, rows).transpose(3, 1, 0, 2).reshape(rows * odim, n_seq * ns)
        ib, jb = 8, 128
        wt = w_opm_out.transpose(2, 1, 0).reshape(pd, odim * odim)
        pair_out = pl.pallas_call(
            functools.partial(opm_kernel, odim),
            grid=(res // jb, rows // ib),
            in_specs=[pl.BlockSpec((ib * odim, n_seq * ns), lambda j, i: (i, 0)),
                      pl.BlockSpec((n_seq, odim, ns, jb), lambda j, i: (0, 0, 0, j)),
                      pl.BlockSpec((ib, jb, pd), lambda j, i: (i, j, 0)),
                      pl.BlockSpec((ib, 1, jb), lambda j, i: (i, 0, j)),
                      full(pd, odim * odim), full(1, pd)],
            out_specs=pl.BlockSpec((ib, jb, pd), lambda j, i: (i, j, 0)),
            out_shape=jax.ShapeDtypeStruct((rows, res, pd), BF16),
            scratch_shapes=[pltpu.VMEM((ib // 2, odim * odim, 2 * jb), BF16)] * 2,
            compiler_params=params(dimension_semantics=('arbitrary', 'arbitrary')),
            name='outer_product',
        )(a_own, b_all, pair, ninv.reshape(rows, 1, res), wt, b_opm_out.reshape(1, pd).astype(F32))
        return e3, pair_out

    return jax.shard_map(local_block, mesh=mesh, in_specs=(row_spec, row_spec, row_spec) + (rep_spec,) * 12,
                         out_specs=(row_spec, row_spec), check_vma=False)
```

```python
import functools
import math

import jax
import jax.numpy as jnp
from jax import lax
from jax.experimental import pallas as pl
from jax.experimental.pallas import tpu as pltpu
from jax.sharding import PartitionSpec as P

MASK_FILL = -1e9
LOG2E = math.log2(math.e)
F32 = jnp.float32
BF16 = jnp.bfloat16
VMEM_LIMIT = 62 * 1024 * 1024
MESH = pl.DeviceIdType.MESH
SEQS = 4


def norm_rows(x):
    c = x - jnp.mean(x, axis=0, keepdims=True)
    var = jnp.mean(c * c, axis=0, keepdims=True)
    return (c * lax.rsqrt(var + 1e-5)).astype(BF16)


def dot(a, b):
    return jnp.dot(a, b, preferred_element_type=F32)


def dot_t(a, b):
    return lax.dot_general(a, b, (((1,), (1,)), ((), ())), preferred_element_type=F32)


def sigmoid(x):
    return 1.0 / (1.0 + jnp.exp(-x))


def wide_max(x):
    return jnp.max(jnp.max(x, axis=0, keepdims=True), axis=1, keepdims=True)[0, 0]


def enter(axis, me, n):
    barrier = pltpu.get_barrier_semaphore()
    for t in range(1, n):
        pl.semaphore_signal(barrier, inc=1, device_id={axis: lax.rem(me + t, n)}, device_id_type=MESH)
    pl.semaphore_wait(barrier, n - 1)


def neighbours(me, n):
    return lax.rem(me + 2, n), lax.rem(me + n - 2, n), lax.rem(me + 4, n), me + 1 - 2 * lax.rem(me, 2)


def sender(axis, send_sem, recv_sem):
    def send(k, src, dst, to):
        copy = pltpu.make_async_remote_copy(src_ref=src, dst_ref=dst, send_sem=send_sem.at[k], recv_sem=recv_sem.at[k],
                                            device_id={axis: to}, device_id_type=MESH)
        copy.start()
        return copy
    return send


def gather_open(send, me, n, own, buf):
    right, left, _, other = neighbours(me, n)
    return [send(0, own, buf.at[me], right), send(1, own, buf.at[me], left), send(2, own, buf.at[me], other)]


def gather_pass(send, me, n, buf, half, c):
    right, left, _, other = neighbours(me, n)
    c[0].wait_recv()
    c.append(send(3, buf.at[left, 0:half], buf.at[left, 0:half], right))
    c.append(send(5, buf.at[left], buf.at[left], other))
    c[1].wait_recv()
    c.append(send(4, buf.at[right, half:], buf.at[right, half:], left))
    c.append(send(6, buf.at[right], buf.at[right], other))
    return c


def gather_close(send, me, n, buf, half, c):
    _, _, far, other = neighbours(me, n)
    c[3].wait_recv()
    c.append(send(7, buf.at[far, 0:half], buf.at[far, 0:half], other))
    c[5].wait_recv()
    c.append(send(8, buf.at[far, half:], buf.at[far, half:], other))
    for t in (2, 4, 6, 7, 8):
        c[t].wait_recv()
    for t in c:
        t.wait_send()


def identity(size):
    return (lax.broadcasted_iota(jnp.int32, (size, size), 0) == lax.broadcasted_iota(jnp.int32, (size, size), 1)).astype(BF16)


def bias_kernel(axis, n, z_ref, w_ref, m_ref, out_ref, ninv_ref, cnt_ref, blk_ref, send_sem, recv_sem):
    rows, res, pd = z_ref.shape
    heads = w_ref.shape[0]
    ns = m_ref.shape[0]
    me = lax.axis_index(axis)
    enter(axis, me, n)
    eye = identity(pd)
    tall, step = 16, 4

    def block(ib, _):
        for t in range(tall // step):
            zt = dot_t(eye, z_ref[pl.ds(ib * tall + t * step, step)].reshape(step * res, pd))
            b = dot(w_ref[...], norm_rows(zt))
            for u in range(step):
                blk_ref[:, t * step + u, :] = b[:, u * res:(u + 1) * res]
        for h in range(heads):
            out_ref[me, pl.ds(pl.multiple_of(h * rows + ib * tall, tall), tall), :] = blk_ref[h].astype(BF16)
        return 0

    lax.fori_loop(0, rows // tall, block, 0)
    out_ref[me, heads * rows:, :] = m_ref[...]
    half = out_ref.shape[1] // 2
    send = sender(axis, send_sem, recv_sem)
    c = gather_open(send, me, n, out_ref.at[me], out_ref)
    c = gather_pass(send, me, n, out_ref, half, c)
    gather_close(send, me, n, out_ref, half, c)
    mask = out_ref[:, heads * rows:, :].reshape(n * ns, res)
    pick = (lax.broadcasted_iota(jnp.int32, (rows, res), 1) ==
            lax.broadcasted_iota(jnp.int32, (rows, res), 0) + me * rows).astype(BF16)
    pairs = dot(dot_t(pick, mask).astype(BF16), mask)
    ninv = 1.0 / (pairs + 1e-3)
    for i in range(rows):
        ninv_ref[i] = ninv[i:i + 1]
    cnt_ref[...] = dot(jnp.ones((8, n * ns), BF16), mask)[0:1]


def row_kernel(heads, hd, scale, e_ref, m_ref, packed_ref, win_ref, bg_ref, wout_ref, cin_ref,
               e1_ref, g_ref, kv_ref, qsum_ref, rhs_ref, kaug_ref, va_ref, att_ref, bias_ref, top_ref):
    us, ch, res = e_ref.shape
    ht = heads * hd
    wide = us * res
    step = pl.program_id(0)

    @pl.when(step == 0)
    def _():
        rows = lax.broadcasted_iota(jnp.int32, rhs_ref.shape, 1)
        rhs_ref[...] = jnp.where(rows == 2 * ht, 1.0, 0.0).astype(BF16)
        qsum_ref[...] = jnp.zeros_like(qsum_ref)
        n, rows = packed_ref.shape[0], res // packed_ref.shape[0]
        for h in range(heads):
            one = jnp.concatenate([packed_ref[d, h * rows:(h + 1) * rows, :] for d in range(n)], axis=0)
            bias_ref[h // 2, :, (h % 2) * res:(h % 2 + 1) * res] = jnp.transpose(one.astype(F32)) * LOG2E
        top = jnp.abs(bias_ref[0])
        for pr in range(1, heads // 2):
            top = jnp.maximum(top, jnp.abs(bias_ref[pr]))
        top_ref[0] = wide_max(top)

    x = jnp.concatenate([e_ref[u] for u in range(us)], axis=1).astype(F32)
    proj = dot(win_ref[...], norm_rows(x)).astype(BF16).astype(F32)
    q, k, v, g = (proj[n * ht:(n + 1) * ht] for n in range(4))
    keep = m_ref[0]
    qs = q * (scale * LOG2E)
    q_top = wide_max(jnp.sum((qs * qs).reshape(heads, hd, wide), axis=1))
    k_top = wide_max(jnp.sum((k * k).reshape(heads, hd, wide), axis=1))
    small = (q_top * k_top < 900.0) & (top_ref[0] < 30.0)

    first_half = (lax.broadcasted_iota(jnp.int32, (ht, wide), 0) % 16) < 8
    hi = qs.astype(BF16).astype(F32)
    for n, part in enumerate((hi, qs - hi)):
        even = jnp.where(first_half, part, 0.0).astype(BF16)
        odd = jnp.where(first_half, 0.0, part).astype(BF16)
        for u in range(us):
            for h in range(heads):
                rows = slice(16 * (h // 2), 16 * (h // 2) + 16)
                rhs_ref[u, n * ht + rows.start:n * ht + rows.stop, h * res:(h + 1) * res] = \
                    (odd if h % 2 else even)[rows, u * res:(u + 1) * res]
    pen = jnp.where(lax.broadcasted_iota(jnp.int32, (16, wide), 0) == 0,
                    jnp.broadcast_to(jnp.where(keep > 0, 0.0, -1e30), (16, wide)), 0.0)
    kaug_ref[...] = jnp.transpose(jnp.concatenate([k, k, pen], axis=0)).astype(BF16)
    ones = jnp.where(lax.broadcasted_iota(jnp.int32, (8, wide), 0) == 0, 1.0, 0.0)
    for pr in range(heads // 2):
        va_ref[pr] = jnp.concatenate([v[16 * pr:16 * pr + 8], ones, v[16 * pr + 8:16 * pr + 16], ones], axis=0).astype(BF16)

    @pl.when(small)
    def _():
        for u in range(us):
            cols = slice(u * res, (u + 1) * res)
            for pr in range(heads // 2):
                s = dot(kaug_ref[cols], rhs_ref[u, :, 2 * pr * res:(2 * pr + 2) * res]) + bias_ref[pr]
                o = dot(va_ref[pr, :, cols], jnp.exp2(s).astype(BF16))
                att_ref[16 * pr:16 * pr + 8, cols] = o[0:8, :res] / o[8:9, :res]
                att_ref[16 * pr + 8:16 * pr + 16, cols] = o[16:24, res:] / o[24:25, res:]
            some = jnp.max(keep[:, cols], axis=1, keepdims=True) > 0
            flat = jnp.mean(v[:, cols], axis=1, keepdims=True)
            att_ref[:, cols] = jnp.where(some, att_ref[:, cols], flat)

    @pl.when(jnp.logical_not(small))
    def _():
        def one(t, _):
            u, pr = t // (heads // 2), t % (heads // 2)
            cols = pl.ds(pl.multiple_of(u * res, res), res)
            s = dot(kaug_ref[cols], rhs_ref[u, :, pl.ds(pl.multiple_of(2 * pr * res, 2 * res), 2 * res)]) + bias_ref[pr]
            p = jnp.exp2(s - jnp.max(s, axis=0, keepdims=True)).astype(BF16)
            o = dot(va_ref[pr, :, cols], p)
            att_ref[pl.ds(pl.multiple_of(16 * pr, 16), 8), cols] = o[0:8, :res] / o[8:9, :res]
            att_ref[pl.ds(pl.multiple_of(16 * pr + 8, 8), 8), cols] = o[16:24, res:] / o[24:25, res:]
            return 0

        lax.fori_loop(0, us * (heads // 2), one, 0)

    gated = (sigmoid(g + bg_ref[...]) * att_ref[...]).astype(BF16)
    e1 = (x + dot(wout_ref[...], gated)).astype(BF16)
    e1_ref[0] = e1
    col = dot(cin_ref[...], norm_rows(e1.astype(F32))).astype(BF16)
    part = col[:ht].astype(F32) * keep
    tot = part[:, :res]
    for u in range(1, us):
        tot = tot + part[:, u * res:(u + 1) * res]
    qsum_ref[...] += tot
    g_ref[0] = col[ht:2 * ht]
    kv_ref[0] = col[2 * ht:]


def exchange(axis, me, n, srcs, dst, send_sem, recv_sem):
    copies = []
    for t in range(1, n):
        peer = lax.rem(me + t, n)
        copy = pltpu.make_async_remote_copy(src_ref=srcs(peer), dst_ref=dst.at[me], send_sem=send_sem.at[t],
                                            recv_sem=recv_sem.at[t], device_id={axis: peer}, device_id_type=MESH)
        copy.start()
        copies.append(copy)
    return copies


def col_kernel(axis, n, heads, hd, scale, qsum_ref, cnt_ref, kv_ref, m_ref, o_ref,
               l_ref, qp_ref, qb_ref, st_ref, sp_ref, send_sem, recv_sem):
    ng, _, wide = kv_ref.shape
    res = qsum_ref.shape[1]
    us = wide // res
    ht = heads * hd
    me = lax.axis_index(axis)
    enter(axis, me, n)
    blk = ht // n
    mine = pl.ds(pl.multiple_of(me * blk, blk), blk)
    copies = exchange(axis, me, n, lambda p: qsum_ref.at[pl.ds(pl.multiple_of(p * blk, blk), blk)], qp_ref,
                      send_sem.at[0], recv_sem.at[0])
    qp_ref[me] = qsum_ref[mine]
    for c in copies:
        c.wait()
    tot = qp_ref[0]
    for t in range(1, n):
        tot = tot + qp_ref[t]
    qb_ref[me] = (tot / (cnt_ref[...] + 1e-10)).astype(BF16).astype(F32)
    copies = exchange(axis, me, n, lambda p: qb_ref.at[me], qb_ref, send_sem.at[1], recv_sem.at[1])
    for c in copies:
        c.wait()
    qbar = qb_ref[...].reshape(ht, res)

    def logits(gr, top):
        for u in range(us):
            cols = slice(u * res, (u + 1) * res)
            kv = kv_ref[gr, :, cols].astype(F32)
            acc = qbar[0:heads] * kv[0:1]
            for d in range(1, hd):
                acc = acc + qbar[d * heads:(d + 1) * heads] * kv[d:d + 1]
            acc = jnp.where(m_ref[gr, :, cols] > 0, acc * scale, MASK_FILL)
            l_ref[gr, :, cols] = acc
            top = jnp.maximum(top, acc)
        return top

    top = lax.fori_loop(0, ng, logits, jnp.full((heads, res), -3e38, F32))

    def sums(gr, carry):
        for u in range(us):
            cols = slice(u * res, (u + 1) * res)
            w = jnp.exp(l_ref[gr, :, cols] - top)
            kv = kv_ref[gr, :, cols].astype(F32)
            carry = (carry[0] + w,) + tuple(carry[1 + d] + w * kv[hd + d:hd + d + 1] for d in range(hd))
        return carry

    zero = jnp.zeros((heads, res), F32)
    tot = lax.fori_loop(0, ng, sums, (zero,) * (hd + 1))
    for d in range(hd):
        st_ref[:, d, :] = tot[1 + d]
    st_ref[:, hd, :] = tot[0]
    st_ref[:, hd + 1, :] = top
    for d in range(hd + 2, st_ref.shape[1]):
        st_ref[:, d, :] = zero
    copies = exchange(axis, me, n, lambda p: st_ref.at[p], sp_ref, send_sem.at[2], recv_sem.at[2])
    sp_ref[me] = st_ref[me]
    for c in copies:
        c.wait()
    best = sp_ref[0, hd + 1:hd + 2]
    for t in range(1, n):
        best = jnp.maximum(best, sp_ref[t, hd + 1:hd + 2])
    num = jnp.zeros((hd, res), F32)
    den = jnp.zeros((1, res), F32)
    for t in range(n):
        fac = jnp.exp(sp_ref[t, hd + 1:hd + 2] - best)
        num = num + sp_ref[t, 0:hd] * fac
        den = den + sp_ref[t, hd:hd + 1] * fac
    o_ref[me] = num / den
    copies = exchange(axis, me, n, lambda p: o_ref.at[me], o_ref, send_sem.at[3], recv_sem.at[3])
    for c in copies:
        c.wait()


def tail_kernel(rows, o_ref, e1_ref, g_ref, m_ref, bg_ref, wout_ref, tin_ref, tout_ref, opm_ref,
                e3_ref, a_ref, b_ref, buf_ref):
    ht, res = o_ref.shape
    us = e1_ref.shape[2] // res
    tb = e3_ref.shape[0]
    chips, odim, _, blk = a_ref.shape
    o = jnp.concatenate([o_ref[...]] * us, axis=1)
    for gr in range(e1_ref.shape[0]):
        gated = (sigmoid(g_ref[gr].astype(F32) + bg_ref[...]) * o).astype(BF16)
        e2 = (e1_ref[gr].astype(F32) + dot(wout_ref[...], gated)).astype(BF16).astype(F32)
        hid = jnp.maximum(dot(tin_ref[...], norm_rows(e2)), 0.0).astype(BF16)
        e3 = (e2 + dot(tout_ref[...], hid)).astype(BF16)
        ab = dot(opm_ref[...], norm_rows(e3.astype(F32))).astype(BF16).astype(F32) * m_ref[gr]
        for u in range(us):
            cols = slice(u * res, (u + 1) * res)
            e3_ref[gr * us + u] = e3[:, cols]
            buf_ref[:, gr * us + u, :] = ab[:, cols]
    for t in range(res // blk):
        b_ref[t] = buf_ref[odim:, :, t * blk:(t + 1) * blk].astype(BF16)
    src = lax.broadcasted_iota(jnp.int32, (res, chips * blk), 0)
    dst = lax.broadcasted_iota(jnp.int32, (res, chips * blk), 1)
    half = blk // 2
    place = ((dst % half < rows) & (src == (dst // half) * rows + dst % half)).astype(BF16)
    moved = dot(buf_ref[0:odim].astype(BF16).reshape(odim * tb, res), place).astype(BF16)
    for c in range(chips):
        a_ref[c] = moved[:, c * blk:(c + 1) * blk].reshape(odim, tb, blk)


def opm_kernel(axis, n, a_ref, b_ref, z_ref, ninv_ref, w_ref, bo_ref, out_ref,
               ag_ref, tr_ref, bg_ref, at_ref, hi_ref, lo_ref, asend, arecv, bsend, brecv):
    rows, res, pd = z_ref.shape
    nb, odim, ns, jb = b_ref.shape
    chips = a_ref.shape[0]
    ib = 2 * hi_ref.shape[0]
    me = lax.axis_index(axis)
    chip, core = me // 2, lax.rem(me, 2)
    right, left, far, other = neighbours(me, n)
    enter(axis, me, n)
    half = odim // 2
    sa = sender(axis, asend, arecv)
    sb = [sender(axis, bsend.at[t], brecv.at[t]) for t in range(nb)]
    up, down, across = lax.rem(chip + 1, chips), lax.rem(chip + chips - 1, chips), lax.rem(chip + 2, chips)
    ca = [sa(2, a_ref.at[across, 0:half], tr_ref.at[0], right), sa(3, a_ref.at[across, half:], tr_ref.at[1], left),
          sa(0, a_ref.at[up], ag_ref.at[me], right), sa(1, a_ref.at[down], ag_ref.at[me], left),
          sa(4, a_ref.at[chip], ag_ref.at[me], other)]
    cb = [gather_open(sb[0], me, n, b_ref.at[0], bg_ref.at[0])]
    ag_ref[me] = a_ref[chip]
    for t in range(nb):
        bg_ref[t, me] = b_ref[t]
    ca[0].wait_recv()
    ca.append(sa(5, tr_ref.at[0], ag_ref.at[left, 0:half], right))
    ca[1].wait_recv()
    ca.append(sa(6, tr_ref.at[1], ag_ref.at[right, half:], left))
    ca[2].wait_recv()
    ca.append(sa(7, ag_ref.at[left], ag_ref.at[left], other))
    ca[3].wait_recv()
    ca.append(sa(8, ag_ref.at[right], ag_ref.at[right], other))
    cb[0] = gather_pass(sb[0], me, n, bg_ref.at[0], half, cb[0])
    cb.append(gather_open(sb[1], me, n, b_ref.at[1], bg_ref.at[1]))
    ca[5].wait_recv()
    ca.append(sa(9, ag_ref.at[far, 0:half], ag_ref.at[far, 0:half], other))
    ca[6].wait_recv()
    ca.append(sa(10, ag_ref.at[far, half:], ag_ref.at[far, half:], other))
    for t in (4, 7, 8, 9, 10):
        ca[t].wait_recv()
    pick = (lax.broadcasted_iota(jnp.int32, (rows, jb), 1) ==
            lax.broadcasted_iota(jnp.int32, (rows, jb), 0) + core * (jb // 2)).astype(BF16)
    for c in range(odim):
        at_ref[:, c, :] = dot_t(pick, ag_ref[:, c].reshape(n * ns, jb))

    def tile(t):
        cols = slice(t * jb, (t + 1) * jb)

        def body(k, _):
            base = k * ib
            a = at_ref[pl.ds(base, ib)].reshape(ib * odim, n * ns).astype(BF16)
            for q in range(odim // 2):
                rhs = jnp.concatenate([bg_ref[t, :, 2 * q].reshape(n * ns, jb), bg_ref[t, :, 2 * q + 1].reshape(n * ns, jb)], axis=1)
                pr = dot(a, rhs)
                hi = pr.astype(BF16)
                lo = (pr - hi.astype(F32)).astype(BF16)
                for val, ref in ((hi, hi_ref), (lo, lo_ref)):
                    for i in range(ib):
                        for h in range(2):
                            ref[i // 2, (2 * q + h) * odim:(2 * q + h + 1) * odim, (i % 2) * jb:(i % 2 + 1) * jb] = \
                                val[i * odim:(i + 1) * odim, h * jb:(h + 1) * jb]
            for ip in range(ib // 2):
                zt = dot(w_ref[...], hi_ref[ip]) + dot(w_ref[...], lo_ref[ip])
                for h in range(2):
                    i = base + 2 * ip + h
                    upd = jnp.transpose(zt[:, h * jb:(h + 1) * jb] * ninv_ref[i, :, cols])
                    out_ref[i, cols, :] = (z_ref[i, cols, :].astype(F32) + upd + bo_ref[...]).astype(BF16)
            return 0

        lax.fori_loop(0, rows // ib, body, 0)

    gather_close(sb[0], me, n, bg_ref.at[0], half, cb[0])
    for t in range(1, nb):
        if t + 1 < nb:
            cb.append(gather_open(sb[t + 1], me, n, b_ref.at[t + 1], bg_ref.at[t + 1]))
        tile(t - 1)
        cb[t] = gather_pass(sb[t], me, n, bg_ref.at[t], half, cb[t])
        gather_close(sb[t], me, n, bg_ref.at[t], half, cb[t])
    tile(nb - 1)
    for t in ca:
        t.wait_send()


def solution(mesh):
    row_spec = P(('batch', 'seq'))
    rep_spec = P()
    n_seq = mesh.shape['seq']

    def local_block(msa, mask, pair, w_pair_bias, w_row_in, b_row_gate, w_row_out, w_col_in, b_col_gate, w_col_out,
                    w_trans_in, w_trans_out, w_opm_in, w_opm_out, b_opm_out):
        ns, res, ch = msa.shape
        rows = pair.shape[0]
        pd = pair.shape[-1]
        heads = w_pair_bias.shape[1]
        ht = w_row_out.shape[0]
        hd = ht // heads
        odim = w_opm_out.shape[0]
        scale = hd ** -0.5
        params = functools.partial(pltpu.CompilerParams, vmem_limit_bytes=VMEM_LIMIT)

        vm = pl.BlockSpec(memory_space=pltpu.VMEM)
        width = heads * rows + ns
        packed, ninv, counts = pl.pallas_call(
            functools.partial(bias_kernel, 'seq', n_seq),
            in_specs=[vm] * 3,
            out_specs=[vm] * 3,
            out_shape=[jax.ShapeDtypeStruct((n_seq, width, res), BF16), jax.ShapeDtypeStruct((rows, 1, res), F32),
                       jax.ShapeDtypeStruct((1, res), F32)],
            scratch_shapes=[pltpu.VMEM((heads, 16, res), F32), pltpu.SemaphoreType.DMA((9,)), pltpu.SemaphoreType.DMA((9,))],
            compiler_params=params(collective_id=1, has_side_effects=True),
            name='pair_bias',
        )(pair, w_pair_bias.T, mask.astype(BF16))

        us = SEQS
        ng, wide = ns // us, us * res
        mask_f = mask.astype(F32).reshape(ng, 1, wide)
        perm_q = w_col_in[:, :ht].reshape(ch, heads, hd).transpose(0, 2, 1).reshape(ch, ht)
        cin = jnp.concatenate([perm_q, w_col_in[:, ht:]], axis=1).T
        ncol = cin.shape[0]
        bcg = b_col_gate.reshape(ht, 1).astype(F32)
        brg = b_row_gate.reshape(ht, 1).astype(F32)

        full = lambda *shape: pl.BlockSpec(shape, lambda *g: (0,) * len(shape))
        group = lambda k, r: pl.BlockSpec((k, r, wide), lambda s: (s, 0, 0))
        e1, gate, kv, qsum = pl.pallas_call(
            functools.partial(row_kernel, heads, hd, scale),
            grid=(ng,),
            in_specs=[pl.BlockSpec((us, ch, res), lambda s: (s, 0, 0)), group(1, 1),
                      full(n_seq, width, res), full(4 * ht, ch), full(ht, 1), full(ch, ht), full(ncol, ch)],
            out_specs=[group(1, ch), group(1, ht), group(1, 2 * hd), full(ht, res)],
            out_shape=[jax.ShapeDtypeStruct((ng, ch, wide), BF16), jax.ShapeDtypeStruct((ng, ht, wide), BF16),
                       jax.ShapeDtypeStruct((ng, 2 * hd, wide), BF16), jax.ShapeDtypeStruct((ht, res), F32)],
            scratch_shapes=[pltpu.VMEM((us, 2 * ht + 16, heads * res), BF16), pltpu.VMEM((wide, 2 * ht + 16), BF16),
                            pltpu.VMEM((heads // 2, 32, wide), BF16), pltpu.VMEM((ht, wide), F32),
                            pltpu.VMEM((heads // 2, res, 2 * res), F32), pltpu.SMEM((1,), F32)],
            compiler_params=params(dimension_semantics=('arbitrary',)),
            name='row_attention',
        )(jnp.transpose(msa, (0, 2, 1)), mask_f, packed, w_row_in.T, brg, w_row_out.T, cin)

        col_o = pl.pallas_call(
            functools.partial(col_kernel, 'seq', n_seq, heads, hd, scale),
            in_specs=[pl.BlockSpec(memory_space=pltpu.VMEM)] * 4,
            out_specs=pl.BlockSpec(memory_space=pltpu.VMEM),
            out_shape=jax.ShapeDtypeStruct((heads, hd, res), F32),
            scratch_shapes=[pltpu.VMEM((ng, heads, wide), F32), pltpu.VMEM((n_seq, ht // n_seq, res), F32),
                            pltpu.VMEM((n_seq, ht // n_seq, res), F32), pltpu.VMEM((heads, 16, res), F32),
                            pltpu.VMEM((n_seq, 16, res), F32), pltpu.SemaphoreType.DMA((4, n_seq)),
                            pltpu.SemaphoreType.DMA((4, n_seq))],
            compiler_params=params(collective_id=0, has_side_effects=True),
            name='col_stats',
        )(qsum, counts, kv, mask_f).reshape(ht, res)

        tb, jb, ib = 16, 128, 8
        chips = n_seq // 2
        e3, a_part, b_part = pl.pallas_call(
            functools.partial(tail_kernel, rows),
            grid=(ns // tb,),
            in_specs=[full(ht, res), group(tb // us, ch), group(tb // us, ht), group(tb // us, 1),
                      full(ht, 1), full(ch, ht), full(w_trans_in.shape[1], ch), full(ch, w_trans_in.shape[1]),
                      full(2 * odim, ch)],
            out_specs=[pl.BlockSpec((tb, ch, res), lambda s: (s, 0, 0)),
                       pl.BlockSpec((chips, odim, tb, jb), lambda s: (0, 0, s, 0)),
                       pl.BlockSpec((res // jb, odim, tb, jb), lambda s: (0, 0, s, 0))],
            out_shape=[jax.ShapeDtypeStruct((ns, ch, res), BF16), jax.ShapeDtypeStruct((chips, odim, ns, jb), BF16),
                       jax.ShapeDtypeStruct((res // jb, odim, ns, jb), BF16)],
            scratch_shapes=[pltpu.VMEM((2 * odim, tb, res), F32)],
            compiler_params=params(dimension_semantics=('arbitrary',)),
            name='tail',
        )(col_o, e1, gate, mask_f, bcg, w_col_out.T, w_trans_in.T, w_trans_out.T, w_opm_in.T)

        wt = w_opm_out.transpose(2, 1, 0).reshape(pd, odim * odim)
        pair_out = pl.pallas_call(
            functools.partial(opm_kernel, 'seq', n_seq),
            in_specs=[vm] * 6,
            out_specs=vm,
            out_shape=jax.ShapeDtypeStruct((rows, res, pd), BF16),
            scratch_shapes=[pltpu.VMEM((n_seq, odim, ns, jb), BF16), pltpu.VMEM((2, odim // 2, ns, jb), BF16),
                            pltpu.VMEM((res // jb, n_seq, odim, ns, jb), BF16), pltpu.VMEM((rows, odim, n_seq * ns), F32),
                            pltpu.VMEM((ib // 2, odim * odim, 2 * jb), BF16), pltpu.VMEM((ib // 2, odim * odim, 2 * jb), BF16),
                            pltpu.SemaphoreType.DMA((11,)), pltpu.SemaphoreType.DMA((11,)),
                            pltpu.SemaphoreType.DMA((res // jb, 9)), pltpu.SemaphoreType.DMA((res // jb, 9))],
            compiler_params=params(collective_id=2, has_side_effects=True),
            name='outer_product',
        )(a_part, b_part, pair, ninv, wt, b_opm_out.reshape(1, pd).astype(F32))
        return jnp.transpose(e3, (0, 2, 1)), pair_out

    return jax.shard_map(local_block, mesh=mesh, in_specs=(row_spec, row_spec, row_spec) + (rep_spec,) * 12,
                         out_specs=(row_spec, row_spec), check_vma=False)
```

```python
import functools
import math

import jax
import jax.numpy as jnp
from jax import lax
from jax.experimental import pallas as pl
from jax.experimental.pallas import tpu as pltpu
from jax.sharding import PartitionSpec as P

MASK_FILL = -1e9
LOG2E = math.log2(math.e)
F32 = jnp.float32
BF16 = jnp.bfloat16
VMEM_LIMIT = 62 * 1024 * 1024
MESH = pl.DeviceIdType.MESH
SEQS = 4


def norm_rows(x):
    c = x - jnp.mean(x, axis=0, keepdims=True)
    var = jnp.mean(c * c, axis=0, keepdims=True)
    return (c * lax.rsqrt(var + 1e-5)).astype(BF16)


def dot(a, b):
    return jnp.dot(a, b, preferred_element_type=F32)


def dot_t(a, b):
    return lax.dot_general(a, b, (((1,), (1,)), ((), ())), preferred_element_type=F32)


def sigmoid(x):
    return 1.0 / (1.0 + jnp.exp(-x))


def wide_max(x):
    return jnp.max(jnp.max(x, axis=0, keepdims=True), axis=1, keepdims=True)[0, 0]


def enter(axis, me, n):
    barrier = pltpu.get_barrier_semaphore()
    for t in range(1, n):
        pl.semaphore_signal(barrier, inc=1, device_id={axis: lax.rem(me + t, n)}, device_id_type=MESH)
    pl.semaphore_wait(barrier, n - 1)


def neighbours(me, n):
    return lax.rem(me + 2, n), lax.rem(me + n - 2, n), lax.rem(me + 4, n), me + 1 - 2 * lax.rem(me, 2)


def remote(axis, sems, src, dst, to):
    return pltpu.make_async_remote_copy(src_ref=src, dst_ref=dst, send_sem=sems[0], recv_sem=sems[1],
                                        device_id={axis: to}, device_id_type=MESH)


class Gather:
    def __init__(self, axis, me, n, sems, own, view):
        right, left, far, other = neighbours(me, n)
        plan = [(own, view(me), right), (own, view(me), left), (own, view(me), other),
                (view(left, 0), view(left, 0), right), (view(right, 1), view(right, 1), left),
                (view(left), view(left), other), (view(right), view(right), other),
                (view(far, 0), view(far, 0), other), (view(far, 1), view(far, 1), other)]
        self.copy = lambda k: remote(axis, sems(k), *plan[k])

    def after(self, waits, starts):
        for k in waits:
            self.copy(k).wait_recv()
        for k in starts:
            self.copy(k).start()

    def open(self):
        self.after((), (0, 1, 2))

    def hand_on(self):
        self.after((0,), (3, 5))
        self.after((1,), (4, 6))

    def close(self):
        self.after((3,), (7,))
        self.after((4,), (8,))
        self.after((2, 5, 6, 7, 8), ())
        for k in range(9):
            self.copy(k).wait_send()


def identity(size):
    return (lax.broadcasted_iota(jnp.int32, (size, size), 0) == lax.broadcasted_iota(jnp.int32, (size, size), 1)).astype(BF16)


def flip(x):
    return jnp.transpose(x.astype(F32)).astype(BF16)


def column(row):
    k = row.shape[1]
    on = lax.broadcasted_iota(jnp.int32, (k, k), 0) == lax.broadcasted_iota(jnp.int32, (k, k), 1)
    return jnp.sum(jnp.where(on, jnp.broadcast_to(row.astype(F32), (k, k)), 0.0), axis=1, keepdims=True)


def mask_row(m_ref, first, count):
    return jnp.concatenate([m_ref[pl.ds(first + u, 1), :] for u in range(count)], axis=1).astype(F32)


def bias_kernel(axis, n, z_hbm, w_ref, m_ref, out_ref, mask_ref, ninv_ref, cnt_ref, z_ref, blk_ref, local, send_sem, recv_sem):
    rows, res, pd = z_ref.shape
    heads = w_ref.shape[0]
    nblk, tall = out_ref.shape[1], out_ref.shape[3]
    ns = m_ref.shape[0]
    step = 4
    me = lax.axis_index(axis)

    def fetch(ib):
        at = pl.ds(ib * tall, tall)
        return pltpu.make_async_copy(z_hbm.at[at], z_ref.at[at], local.at[ib])

    for ib in range(nblk):
        fetch(ib).start()
    mask_ref[me] = m_ref[...].astype(BF16)
    enter(axis, me, n)
    hh, hs = heads // 2, ns // 2
    sems = lambda t: lambda k: (send_sem.at[t, k], recv_sem.at[t, k])
    mask_ring = Gather(axis, me, n, sems(nblk), mask_ref.at[me],
                       lambda d, p=None: mask_ref.at[d] if p is None else mask_ref.at[d, pl.ds(p * hs, hs)])

    def ring(ib):
        return Gather(axis, me, n, sems(ib), out_ref.at[me, ib],
                      lambda d, p=None: out_ref.at[d, ib] if p is None else out_ref.at[d, ib, pl.ds(p * hh, hh)])

    mask_ring.open()
    eye = identity(pd)

    def block(ib, _):
        fetch(ib).wait()
        for t in range(tall // step):
            zt = dot_t(eye, z_ref[pl.ds(ib * tall + t * step, step)].reshape(step * res, pd))
            b = dot(w_ref[...], norm_rows(zt))
            for u in range(step):
                blk_ref[:, t * step + u, :] = b[:, u * res:(u + 1) * res]
        out_ref[me, ib] = blk_ref[...].astype(BF16)
        ring(ib).open()
        return 0

    lax.fori_loop(0, nblk, block, 0)
    mask_ring.hand_on()
    for ib in range(nblk):
        ring(ib).hand_on()
    mask_ring.close()
    mask = mask_ref[...].reshape(n * ns, res)
    pick = (lax.broadcasted_iota(jnp.int32, (rows, res), 1) ==
            lax.broadcasted_iota(jnp.int32, (rows, res), 0) + me * rows).astype(BF16)
    pairs = dot(dot_t(pick, mask).astype(BF16), mask)
    ninv = 1.0 / (pairs + 1e-3)
    for i in range(rows):
        ninv_ref[i] = ninv[i:i + 1]
    cnt_ref[...] = dot(jnp.ones((8, n * ns), BF16), mask)[0:1]
    for ib in range(nblk):
        ring(ib).close()


def row_kernel(heads, hd, scale, e_ref, m_ref, packed_ref, win_ref, bg_ref, wout_ref, cin_ref,
               e1_ref, g_ref, kv_ref, qsum_ref,
               rhs_ref, kaug_ref, va_ref, att_ref, bias_ref, wt_ref, ot_ref, ct_ref, gb_ref, top_ref):
    us, ch, res = e_ref.shape
    ht = heads * hd
    wide = us * res
    step = pl.program_id(0)

    @pl.when(step == 0)
    def _():
        rows = lax.broadcasted_iota(jnp.int32, rhs_ref.shape, 1)
        rhs_ref[...] = jnp.where(rows == 2 * ht, 1.0, 0.0).astype(BF16)
        qsum_ref[...] = jnp.zeros_like(qsum_ref)
        wt_ref[...] = flip(win_ref[...])
        ot_ref[...] = flip(wout_ref[...])
        ct = flip(cin_ref[...])
        r = lax.broadcasted_iota(jnp.int32, (ht, ht), 0)
        turn = (lax.broadcasted_iota(jnp.int32, (ht, ht), 1) == lax.rem(r, heads) * hd + r // heads).astype(BF16)
        ct_ref[...] = jnp.concatenate([dot(turn, ct[:ht]).astype(BF16), ct[ht:]], axis=0)
        gb_ref[...] = column(bg_ref[...])
        for h in range(heads):
            one = jnp.concatenate([packed_ref[d, t, h] for d in range(packed_ref.shape[0])
                                   for t in range(packed_ref.shape[1])], axis=0)
            bias_ref[h // 2, :, (h % 2) * res:(h % 2 + 1) * res] = jnp.transpose(one.astype(F32)) * LOG2E
        top = jnp.abs(bias_ref[0])
        for pr in range(1, heads // 2):
            top = jnp.maximum(top, jnp.abs(bias_ref[pr]))
        top_ref[0] = wide_max(top)

    x = jnp.concatenate([e_ref[u] for u in range(us)], axis=1).astype(F32)
    proj = dot(wt_ref[...], norm_rows(x)).astype(BF16).astype(F32)
    q, k, v, g = (proj[n * ht:(n + 1) * ht] for n in range(4))
    keep = mask_row(m_ref, step * us, us)
    qs = q * (scale * LOG2E)
    q_top = wide_max(jnp.sum((qs * qs).reshape(heads, hd, wide), axis=1))
    k_top = wide_max(jnp.sum((k * k).reshape(heads, hd, wide), axis=1))
    small = (q_top * k_top < 900.0) & (top_ref[0] < 30.0)

    first_half = (lax.broadcasted_iota(jnp.int32, (ht, wide), 0) % 16) < 8
    hi = qs.astype(BF16).astype(F32)
    for n, part in enumerate((hi, qs - hi)):
        even = jnp.where(first_half, part, 0.0).astype(BF16)
        odd = jnp.where(first_half, 0.0, part).astype(BF16)
        for u in range(us):
            for h in range(heads):
                rows = slice(16 * (h // 2), 16 * (h // 2) + 16)
                rhs_ref[u, n * ht + rows.start:n * ht + rows.stop, h * res:(h + 1) * res] = \
                    (odd if h % 2 else even)[rows, u * res:(u + 1) * res]
    pen = jnp.where(lax.broadcasted_iota(jnp.int32, (16, wide), 0) == 0,
                    jnp.broadcast_to(jnp.where(keep > 0, 0.0, -1e30), (16, wide)), 0.0)
    kaug_ref[...] = jnp.transpose(jnp.concatenate([k, k, pen], axis=0)).astype(BF16)
    ones = jnp.where(lax.broadcasted_iota(jnp.int32, (8, wide), 0) == 0, 1.0, 0.0)
    for pr in range(heads // 2):
        va_ref[pr] = jnp.concatenate([v[16 * pr:16 * pr + 8], ones, v[16 * pr + 8:16 * pr + 16], ones], axis=0).astype(BF16)

    @pl.when(small)
    def _():
        for u in range(us):
            cols = slice(u * res, (u + 1) * res)
            for pr in range(heads // 2):
                s = dot(kaug_ref[cols], rhs_ref[u, :, 2 * pr * res:(2 * pr + 2) * res]) + bias_ref[pr]
                o = dot(va_ref[pr, :, cols], jnp.exp2(s).astype(BF16))
                att_ref[16 * pr:16 * pr + 8, cols] = o[0:8, :res] / o[8:9, :res]
                att_ref[16 * pr + 8:16 * pr + 16, cols] = o[16:24, res:] / o[24:25, res:]
            some = jnp.max(keep[:, cols], axis=1, keepdims=True) > 0
            flat = jnp.mean(v[:, cols], axis=1, keepdims=True)
            att_ref[:, cols] = jnp.where(some, att_ref[:, cols], flat)

    @pl.when(jnp.logical_not(small))
    def _():
        def one(t, _):
            u, pr = t // (heads // 2), t % (heads // 2)
            cols = pl.ds(pl.multiple_of(u * res, res), res)
            s = dot(kaug_ref[cols], rhs_ref[u, :, pl.ds(pl.multiple_of(2 * pr * res, 2 * res), 2 * res)]) + bias_ref[pr]
            p = jnp.exp2(s - jnp.max(s, axis=0, keepdims=True)).astype(BF16)
            o = dot(va_ref[pr, :, cols], p)
            att_ref[pl.ds(pl.multiple_of(16 * pr, 16), 8), cols] = o[0:8, :res] / o[8:9, :res]
            att_ref[pl.ds(pl.multiple_of(16 * pr + 8, 8), 8), cols] = o[16:24, res:] / o[24:25, res:]
            return 0

        lax.fori_loop(0, us * (heads // 2), one, 0)

    gated = (sigmoid(g + gb_ref[...]) * att_ref[...]).astype(BF16)
    e1 = (x + dot(ot_ref[...], gated)).astype(BF16)
    e1_ref[0] = e1
    col = dot(ct_ref[...], norm_rows(e1.astype(F32))).astype(BF16)
    part = col[:ht].astype(F32) * keep
    tot = part[:, :res]
    for u in range(1, us):
        tot = tot + part[:, u * res:(u + 1) * res]
    qsum_ref[...] += tot
    g_ref[0] = col[ht:2 * ht]
    kv_ref[0] = col[2 * ht:]


def exchange(axis, me, n, srcs, dst, send_sem, recv_sem):
    copies = []
    for t in range(1, n):
        peer = lax.rem(me + t, n)
        copy = pltpu.make_async_remote_copy(src_ref=srcs(peer), dst_ref=dst.at[me], send_sem=send_sem.at[t],
                                            recv_sem=recv_sem.at[t], device_id={axis: peer}, device_id_type=MESH)
        copy.start()
        copies.append(copy)
    return copies


def col_kernel(axis, n, heads, hd, scale, qsum_ref, cnt_ref, kv_ref, m_ref, o_ref,
               l_ref, qp_ref, qb_ref, st_ref, sp_ref, send_sem, recv_sem):
    ng, _, wide = kv_ref.shape
    res = qsum_ref.shape[1]
    us = wide // res
    ht = heads * hd
    me = lax.axis_index(axis)
    enter(axis, me, n)
    blk = ht // n
    mine = pl.ds(pl.multiple_of(me * blk, blk), blk)
    copies = exchange(axis, me, n, lambda p: qsum_ref.at[pl.ds(pl.multiple_of(p * blk, blk), blk)], qp_ref,
                      send_sem.at[0], recv_sem.at[0])
    qp_ref[me] = qsum_ref[mine]
    for c in copies:
        c.wait()
    tot = qp_ref[0]
    for t in range(1, n):
        tot = tot + qp_ref[t]
    qb_ref[me] = (tot / (cnt_ref[...] + 1e-10)).astype(BF16).astype(F32)
    copies = exchange(axis, me, n, lambda p: qb_ref.at[me], qb_ref, send_sem.at[1], recv_sem.at[1])
    for c in copies:
        c.wait()
    qbar = qb_ref[...].reshape(ht, res)

    def logits(gr, top):
        for u in range(us):
            cols = slice(u * res, (u + 1) * res)
            kv = kv_ref[gr, :, cols].astype(F32)
            acc = qbar[0:heads] * kv[0:1]
            for d in range(1, hd):
                acc = acc + qbar[d * heads:(d + 1) * heads] * kv[d:d + 1]
            acc = jnp.where(m_ref[pl.ds(gr * us + u, 1), :] > 0, acc * scale, MASK_FILL)
            l_ref[gr, :, cols] = acc
            top = jnp.maximum(top, acc)
        return top

    top = lax.fori_loop(0, ng, logits, jnp.full((heads, res), -3e38, F32))

    def sums(gr, carry):
        for u in range(us):
            cols = slice(u * res, (u + 1) * res)
            w = jnp.exp(l_ref[gr, :, cols] - top)
            kv = kv_ref[gr, :, cols].astype(F32)
            carry = (carry[0] + w,) + tuple(carry[1 + d] + w * kv[hd + d:hd + d + 1] for d in range(hd))
        return carry

    zero = jnp.zeros((heads, res), F32)
    tot = lax.fori_loop(0, ng, sums, (zero,) * (hd + 1))
    for d in range(hd):
        st_ref[:, d, :] = tot[1 + d]
    st_ref[:, hd, :] = tot[0]
    st_ref[:, hd + 1, :] = top
    for d in range(hd + 2, st_ref.shape[1]):
        st_ref[:, d, :] = zero
    copies = exchange(axis, me, n, lambda p: st_ref.at[p], sp_ref, send_sem.at[2], recv_sem.at[2])
    sp_ref[me] = st_ref[me]
    for c in copies:
        c.wait()
    best = sp_ref[0, hd + 1:hd + 2]
    for t in range(1, n):
        best = jnp.maximum(best, sp_ref[t, hd + 1:hd + 2])
    num = jnp.zeros((hd, res), F32)
    den = jnp.zeros((1, res), F32)
    for t in range(n):
        fac = jnp.exp(sp_ref[t, hd + 1:hd + 2] - best)
        num = num + sp_ref[t, 0:hd] * fac
        den = den + sp_ref[t, hd:hd + 1] * fac
    o_ref[me] = num / den
    copies = exchange(axis, me, n, lambda p: o_ref.at[me], o_ref, send_sem.at[3], recv_sem.at[3])
    for c in copies:
        c.wait()


def tail_kernel(axis, n, o_ref, e1_hbm, g_hbm, m_ref, bg_ref, wout_ref, tin_ref, tout_ref, opm_ref,
                z_hbm, ninv_ref, w_ref, bo_ref, e3_hbm, out_hbm,
                e1_ref, g_ref, e3_ref, z_ref, buf_ref, a_ref, b_ref, ag_ref, tr_ref, bg_all, at_ref, hi_ref, lo_ref,
                wp_ref, wf_ref, local, asend, arecv, bsend, brecv):
    rows, res, pd = z_ref.shape
    nb, odim, ns, jb = b_ref.shape
    chips = a_ref.shape[0]
    ht = o_ref.shape[0]
    wide = e1_ref.shape[2]
    us = wide // res
    tb = buf_ref.shape[1]
    ngr = ns // tb
    per = tb // us
    ib = 2 * hi_ref.shape[0]
    half = odim // 2
    me = lax.axis_index(axis)
    chip, core = me // 2, lax.rem(me, 2)
    right, left, far, other = neighbours(me, n)
    up, down, across = lax.rem(chip + 1, chips), lax.rem(chip + chips - 1, chips), lax.rem(chip + 2, chips)

    def fetch(g):
        at = pl.ds(g * per, per)
        return [pltpu.make_async_copy(e1_hbm.at[at], e1_ref.at[at], local.at[0, g]),
                pltpu.make_async_copy(g_hbm.at[at], g_ref.at[at], local.at[1, g])]

    for g in range(ngr):
        for c in fetch(g):
            c.start()
    z_in = pltpu.make_async_copy(z_hbm, z_ref, local.at[2, 0])
    z_in.start()
    enter(axis, me, n)

    part = {None: slice(None), 0: pl.ds(0, half), 1: pl.ds(half, half)}

    def a_copies(g):
        seqs = pl.ds(pl.multiple_of(g * tb, tb), tb)
        src = lambda c, p=None: a_ref.at[c, part[p], seqs]
        dst = lambda d, p=None: ag_ref.at[d, part[p], seqs]
        tr = lambda t: tr_ref.at[t, :, seqs]
        plan = [(src(across, 0), tr(0), right), (src(across, 1), tr(1), left), (src(up), dst(me), right),
                (src(down), dst(me), left), (src(chip), dst(me), other),
                (tr(0), dst(left, 0), right), (tr(1), dst(right, 1), left),
                (dst(left), dst(left), other), (dst(right), dst(right), other),
                (dst(far, 0), dst(far, 0), other), (dst(far, 1), dst(far, 1), other)]
        return lambda k: remote(axis, (asend.at[g, k], arecv.at[g, k]), *plan[k])

    def b_first(g):
        seqs = pl.ds(pl.multiple_of(g * tb, tb), tb)
        return Gather(axis, me, n, lambda k: (bsend.at[g, k], brecv.at[g, k]), b_ref.at[0, :, seqs],
                      lambda d, p=None: bg_all.at[0, d, part[p], seqs])

    def b_rest(t):
        return Gather(axis, me, n, lambda k: (bsend.at[ngr - 1 + t, k], brecv.at[ngr - 1 + t, k]), b_ref.at[t],
                      lambda d, p=None: bg_all.at[t, d] if p is None else bg_all.at[t, d, part[p]])

    src = lax.broadcasted_iota(jnp.int32, (res, chips * jb), 0)
    dst = lax.broadcasted_iota(jnp.int32, (res, chips * jb), 1)
    hj = jb // 2
    place = ((dst % hj < rows) & (src == (dst // hj) * rows + dst % hj)).astype(BF16)

    wout, tin, opm = (flip(r[...]) for r in (wout_ref, tin_ref, opm_ref))
    gate_bias = column(bg_ref[...])

    def group(g, _):
        seqs = pl.ds(pl.multiple_of(g * tb, tb), tb)
        for c in fetch(g):
            c.wait()
        o = jnp.concatenate([o_ref[...]] * us, axis=1)
        for j in range(per):
            gr = g * per + j
            gated = (sigmoid(g_ref[gr].astype(F32) + gate_bias) * o).astype(BF16)
            e2 = (e1_ref[gr].astype(F32) + dot(wout, gated)).astype(BF16).astype(F32)
            hid = jnp.maximum(dot(tin, norm_rows(e2)), 0.0).astype(BF16)
            e3 = (e2 + dot(tout_ref[...], hid)).astype(BF16)
            ab = dot(opm, norm_rows(e3.astype(F32))).astype(BF16).astype(F32) * mask_row(m_ref, gr * us, us)
            for u in range(us):
                cols = slice(u * res, (u + 1) * res)
                e3_ref[gr * us + u] = e3[:, cols]
                buf_ref[:, j * us + u, :] = ab[:, cols]
        moved = dot(buf_ref[0:odim].astype(BF16).reshape(odim * tb, res), place).astype(BF16)
        for c in range(chips):
            a_ref[c, :, seqs, :] = moved[:, c * jb:(c + 1) * jb].reshape(odim, tb, jb)
        for t in range(nb):
            blk = buf_ref[odim:, :, t * jb:(t + 1) * jb].astype(BF16)
            b_ref[t, :, seqs, :] = blk
            bg_all[t, me, :, seqs, :] = blk
        ac = a_copies(g)
        for k in range(5):
            ac(k).start()
        b_first(g).open()
        ag_ref[me, :, seqs, :] = a_ref[chip, :, seqs, :]
        return 0

    lax.fori_loop(0, ngr, group, 0)
    e3_out = pltpu.make_async_copy(e3_ref, e3_hbm, local.at[2, 1])
    e3_out.start()

    def pass_on(g, _):
        ac = a_copies(g)
        for wait, start in ((0, 5), (1, 6), (2, 7), (3, 8)):
            ac(wait).wait_recv()
            ac(start).start()
        b_first(g).hand_on()
        return 0

    lax.fori_loop(0, ngr, pass_on, 0)
    b_rest(1).open()

    def finish_a(g, _):
        ac = a_copies(g)
        for wait, start in ((5, 9), (6, 10)):
            ac(wait).wait_recv()
            ac(start).start()
        for k in (4, 7, 8, 9, 10):
            ac(k).wait_recv()
        for k in range(11):
            ac(k).wait_send()
        return 0

    lax.fori_loop(0, ngr, finish_a, 0)
    wf_ref[...] = w_ref[...].astype(F32)
    for d in range(odim):
        wp_ref[:, d * odim:(d + 1) * odim] = jnp.transpose(wf_ref[:, d, :]).astype(BF16)
    pick = (lax.broadcasted_iota(jnp.int32, (rows, jb), 1) ==
            lax.broadcasted_iota(jnp.int32, (rows, jb), 0) + core * hj).astype(BF16)
    for c in range(odim):
        at_ref[:, c, :] = dot_t(pick, ag_ref[:, c].reshape(n * ns, jb))

    def finish_b(g, _):
        b_first(g).close()
        return 0

    lax.fori_loop(0, ngr, finish_b, 0)
    z_in.wait()
    steps = rows // ib

    def done(t):
        at = pl.ds(t * jb, jb)
        return pltpu.make_async_copy(z_ref.at[:, at], out_hbm.at[:, at], local.at[3, t])

    def body(k, _):
        t = k // steps
        base = lax.rem(k, steps) * ib
        cols = pl.ds(pl.multiple_of(t * jb, jb), jb)

        for later in range(1, nb):
            @pl.when(k == (later - 1) * steps + steps // 2)
            def _():
                b_rest(later).hand_on()
                if later + 1 < nb:
                    b_rest(later + 1).open()

            @pl.when(k == later * steps)
            def _():
                b_rest(later).close()
                done(later - 1).start()

        a = at_ref[pl.ds(base, ib)].reshape(ib * odim, n * ns).astype(BF16)
        for q in range(odim // 2):
            rhs = jnp.concatenate([bg_all[t, :, 2 * q].reshape(n * ns, jb), bg_all[t, :, 2 * q + 1].reshape(n * ns, jb)], axis=1)
            pr = dot(a, rhs)
            hi = pr.astype(BF16)
            lo = (pr - hi.astype(F32)).astype(BF16)
            for val, ref in ((hi, hi_ref), (lo, lo_ref)):
                for i in range(ib):
                    for h in range(2):
                        ref[i // 2, (2 * q + h) * odim:(2 * q + h + 1) * odim, (i % 2) * jb:(i % 2 + 1) * jb] = \
                            val[i * odim:(i + 1) * odim, h * jb:(h + 1) * jb]
        for ip in range(ib // 2):
            zt = dot(wp_ref[...], hi_ref[ip]) + dot(wp_ref[...], lo_ref[ip])
            for h in range(2):
                i = base + 2 * ip + h
                upd = jnp.transpose(zt[:, h * jb:(h + 1) * jb] * ninv_ref[i, :, cols])
                z_ref[i, cols, :] = (z_ref[i, cols, :].astype(F32) + upd + bo_ref[...].astype(F32)).astype(BF16)
        return 0

    lax.fori_loop(0, nb * steps, body, 0)
    done(nb - 1).start()
    for t in range(nb):
        done(t).wait()
    e3_out.wait()


def solution(mesh):
    row_spec = P(('batch', 'seq'))
    rep_spec = P()
    n_seq = mesh.shape['seq']

    def local_block(msa, mask, pair, w_pair_bias, w_row_in, b_row_gate, w_row_out, w_col_in, b_col_gate, w_col_out,
                    w_trans_in, w_trans_out, w_opm_in, w_opm_out, b_opm_out):
        ns, res, ch = msa.shape
        rows = pair.shape[0]
        pd = pair.shape[-1]
        heads = w_pair_bias.shape[1]
        ht = w_row_out.shape[0]
        hd = ht // heads
        odim = w_opm_out.shape[0]
        scale = hd ** -0.5
        params = functools.partial(pltpu.CompilerParams, vmem_limit_bytes=VMEM_LIMIT)

        vm = pl.BlockSpec(memory_space=pltpu.VMEM)
        hbm = pl.BlockSpec(memory_space=pl.ANY)
        dma = pltpu.SemaphoreType.DMA
        tall = 16
        nblk = rows // tall
        packed, _, ninv, counts = pl.pallas_call(
            functools.partial(bias_kernel, 'seq', n_seq),
            in_specs=[hbm, vm, vm],
            out_specs=[vm] * 4,
            out_shape=[jax.ShapeDtypeStruct((n_seq, nblk, heads, tall, res), BF16), jax.ShapeDtypeStruct((n_seq, ns, res), BF16),
                       jax.ShapeDtypeStruct((rows, 1, res), F32), jax.ShapeDtypeStruct((1, res), F32)],
            scratch_shapes=[pltpu.VMEM((rows, res, pd), BF16), pltpu.VMEM((heads, tall, res), F32), dma((nblk,)),
                            dma((nblk + 1, 9)), dma((nblk + 1, 9))],
            compiler_params=params(collective_id=1, has_side_effects=True),
            name='pair_bias',
        )(pair, w_pair_bias.T, mask)

        us = SEQS
        ng, wide = ns // us, us * res
        ncol = w_col_in.shape[1]

        full = lambda *shape: pl.BlockSpec(shape, lambda *g: (0,) * len(shape))
        group = lambda k, r: pl.BlockSpec((k, r, wide), lambda s: (s, 0, 0))
        e1, gate, kv, qsum = pl.pallas_call(
            functools.partial(row_kernel, heads, hd, scale),
            grid=(ng,),
            in_specs=[pl.BlockSpec((us, ch, res), lambda s: (s, 0, 0)), full(ns, res),
                      full(n_seq, nblk, heads, tall, res), full(ch, 4 * ht), full(1, ht), full(ht, ch), full(ch, ncol)],
            out_specs=[group(1, ch), group(1, ht), group(1, 2 * hd), full(ht, res)],
            out_shape=[jax.ShapeDtypeStruct((ng, ch, wide), BF16), jax.ShapeDtypeStruct((ng, ht, wide), BF16),
                       jax.ShapeDtypeStruct((ng, 2 * hd, wide), BF16), jax.ShapeDtypeStruct((ht, res), F32)],
            scratch_shapes=[pltpu.VMEM((us, 2 * ht + 16, heads * res), BF16), pltpu.VMEM((wide, 2 * ht + 16), BF16),
                            pltpu.VMEM((heads // 2, 32, wide), BF16), pltpu.VMEM((ht, wide), F32),
                            pltpu.VMEM((heads // 2, res, 2 * res), F32), pltpu.VMEM((4 * ht, ch), BF16),
                            pltpu.VMEM((ch, ht), BF16), pltpu.VMEM((ncol, ch), BF16), pltpu.VMEM((ht, 1), F32), pltpu.SMEM((1,), F32)],
            compiler_params=params(dimension_semantics=('arbitrary',)),
            name='row_attention',
        )(jnp.transpose(msa, (0, 2, 1)), mask, packed, w_row_in, b_row_gate.reshape(1, ht), w_row_out, w_col_in)

        col_o = pl.pallas_call(
            functools.partial(col_kernel, 'seq', n_seq, heads, hd, scale),
            in_specs=[pl.BlockSpec(memory_space=pltpu.VMEM)] * 4,
            out_specs=pl.BlockSpec(memory_space=pltpu.VMEM),
            out_shape=jax.ShapeDtypeStruct((heads, hd, res), F32),
            scratch_shapes=[pltpu.VMEM((ng, heads, wide), F32), pltpu.VMEM((n_seq, ht // n_seq, res), F32),
                            pltpu.VMEM((n_seq, ht // n_seq, res), F32), pltpu.VMEM((heads, 16, res), F32),
                            pltpu.VMEM((n_seq, 16, res), F32), pltpu.SemaphoreType.DMA((4, n_seq)),
                            pltpu.SemaphoreType.DMA((4, n_seq))],
            compiler_params=params(collective_id=0, has_side_effects=True),
            name='col_stats',
        )(qsum, counts, kv, mask).reshape(ht, res)

        tb, jb, ib = 16, 128, 8
        chips = n_seq // 2
        nb = res // jb
        e3, pair_out = pl.pallas_call(
            functools.partial(tail_kernel, 'seq', n_seq),
            in_specs=[vm, hbm, hbm] + [vm] * 6 + [hbm] + [vm] * 3,
            out_specs=[hbm, hbm],
            out_shape=[jax.ShapeDtypeStruct((ns, ch, res), BF16), jax.ShapeDtypeStruct((rows, res, pd), BF16)],
            scratch_shapes=[pltpu.VMEM((ng, ch, wide), BF16), pltpu.VMEM((ng, ht, wide), BF16), pltpu.VMEM((ns, ch, res), BF16),
                            pltpu.VMEM((rows, res, pd), BF16), pltpu.VMEM((2 * odim, tb, res), F32),
                            pltpu.VMEM((chips, odim, ns, jb), BF16), pltpu.VMEM((nb, odim, ns, jb), BF16),
                            pltpu.VMEM((n_seq, odim, ns, jb), BF16), pltpu.VMEM((2, odim // 2, ns, jb), BF16),
                            pltpu.VMEM((nb, n_seq, odim, ns, jb), BF16), pltpu.VMEM((rows, odim, n_seq * ns), F32),
                            pltpu.VMEM((ib // 2, odim * odim, 2 * jb), BF16), pltpu.VMEM((ib // 2, odim * odim, 2 * jb), BF16),
                            pltpu.VMEM((pd, odim * odim), BF16), pltpu.VMEM((odim, odim, pd), F32),
                            dma((4, max(4, ns // tb))), dma((ns // tb, 11)), dma((ns // tb, 11)),
                            dma((ns // tb + nb - 1, 9)), dma((ns // tb + nb - 1, 9))],
            compiler_params=params(collective_id=2, has_side_effects=True),
            name='tail_outer_product',
        )(col_o, e1, gate, mask, b_col_gate.reshape(1, ht), w_col_out, w_trans_in, w_trans_out.T, w_opm_in,
          pair, ninv, w_opm_out, b_opm_out.reshape(1, pd))
        return jnp.transpose(e3, (0, 2, 1)), pair_out

    return jax.shard_map(local_block, mesh=mesh, in_specs=(row_spec, row_spec, row_spec) + (rep_spec,) * 12,
                         out_specs=(row_spec, row_spec), check_vma=False)
```

```python
import functools
import math

import jax
import jax.numpy as jnp
from jax import lax
from jax.experimental import pallas as pl
from jax.experimental.pallas import tpu as pltpu
from jax.sharding import PartitionSpec as P

MASK_FILL = -1e9
LOG2E = math.log2(math.e)
F32 = jnp.float32
BF16 = jnp.bfloat16
VMEM_LIMIT = 62 * 1024 * 1024
MESH = pl.DeviceIdType.MESH
SEQS = 8


def norm_rows(x):
    c = x - jnp.mean(x, axis=0, keepdims=True)
    var = jnp.mean(c * c, axis=0, keepdims=True)
    return (c * lax.rsqrt(var + 1e-5)).astype(BF16)


def dot(a, b):
    return jnp.dot(a, b, preferred_element_type=F32)


def dot_t(a, b):
    return lax.dot_general(a, b, (((1,), (1,)), ((), ())), preferred_element_type=F32)


def sigmoid(x):
    return 1.0 / (1.0 + jnp.exp(-x))


def wide_max(x):
    return jnp.max(jnp.max(x, axis=0, keepdims=True), axis=1, keepdims=True)[0, 0]


def enter(axis, me, n):
    barrier = pltpu.get_barrier_semaphore()
    for t in range(1, n):
        pl.semaphore_signal(barrier, inc=1, device_id={axis: lax.rem(me + t, n)}, device_id_type=MESH)
    pl.semaphore_wait(barrier, n - 1)


def neighbours(me, n):
    return lax.rem(me + 2, n), lax.rem(me + n - 2, n), lax.rem(me + 4, n), me + 1 - 2 * lax.rem(me, 2)


def remote(axis, sems, src, dst, to):
    return pltpu.make_async_remote_copy(src_ref=src, dst_ref=dst, send_sem=sems[0], recv_sem=sems[1],
                                        device_id={axis: to}, device_id_type=MESH)


class Gather:
    def __init__(self, axis, me, n, sems, own, view):
        right, left, far, other = neighbours(me, n)
        plan = [(own, view(me), right), (own, view(me), left), (own, view(me), other),
                (view(left, 0), view(left, 0), right), (view(right, 1), view(right, 1), left),
                (view(left), view(left), other), (view(right), view(right), other),
                (view(far, 0), view(far, 0), other), (view(far, 1), view(far, 1), other)]
        self.copy = lambda k: remote(axis, sems(k), *plan[k])

    def after(self, waits, starts):
        for k in waits:
            self.copy(k).wait_recv()
        for k in starts:
            self.copy(k).start()

    def open(self):
        self.after((), (0, 1, 2))

    def hand_on(self):
        self.after((0,), (3, 5))
        self.after((1,), (4, 6))

    def close(self):
        self.after((3,), (7,))
        self.after((4,), (8,))
        self.after((2, 5, 6, 7, 8), ())
        for k in range(9):
            self.copy(k).wait_send()


def identity(size):
    return (lax.broadcasted_iota(jnp.int32, (size, size), 0) == lax.broadcasted_iota(jnp.int32, (size, size), 1)).astype(BF16)


def flip(x):
    return jnp.transpose(x.astype(F32)).astype(BF16)


def column(row):
    k = row.shape[1]
    on = lax.broadcasted_iota(jnp.int32, (k, k), 0) == lax.broadcasted_iota(jnp.int32, (k, k), 1)
    return jnp.sum(jnp.where(on, jnp.broadcast_to(row.astype(F32), (k, k)), 0.0), axis=1, keepdims=True)


def mask_row(m_ref, first, count):
    return jnp.concatenate([m_ref[pl.ds(first + u, 1), :] for u in range(count)], axis=1).astype(F32)


def bias_kernel(axis, n, z_hbm, w_ref, m_ref, out_ref, mask_ref, ninv_ref, cnt_ref, z_ref, blk_ref, local, send_sem, recv_sem):
    rows, res, pd = z_ref.shape
    heads = w_ref.shape[0]
    nblk, tall = out_ref.shape[1], out_ref.shape[3]
    ns = m_ref.shape[0]
    step = 4
    me = lax.axis_index(axis)

    def fetch(ib):
        at = pl.ds(ib * tall, tall)
        return pltpu.make_async_copy(z_hbm.at[at], z_ref.at[at], local.at[ib])

    for ib in range(nblk):
        fetch(ib).start()
    mask_ref[me] = m_ref[...].astype(BF16)
    enter(axis, me, n)
    hh, hs = heads // 2, ns // 2
    sems = lambda t: lambda k: (send_sem.at[t, k], recv_sem.at[t, k])
    mask_ring = Gather(axis, me, n, sems(nblk), mask_ref.at[me],
                       lambda d, p=None: mask_ref.at[d] if p is None else mask_ref.at[d, pl.ds(p * hs, hs)])

    def ring(ib):
        return Gather(axis, me, n, sems(ib), out_ref.at[me, ib],
                      lambda d, p=None: out_ref.at[d, ib] if p is None else out_ref.at[d, ib, pl.ds(p * hh, hh)])

    mask_ring.open()
    eye = identity(pd)

    def block(ib, _):
        fetch(ib).wait()
        for t in range(tall // step):
            zt = dot_t(eye, z_ref[pl.ds(ib * tall + t * step, step)].reshape(step * res, pd))
            b = dot(w_ref[...], norm_rows(zt))
            for u in range(step):
                blk_ref[:, t * step + u, :] = b[:, u * res:(u + 1) * res]
        out_ref[me, ib] = blk_ref[...].astype(BF16)
        ring(ib).open()
        return 0

    lax.fori_loop(0, nblk, block, 0)
    mask_ring.hand_on()
    for ib in range(nblk):
        ring(ib).hand_on()
    mask_ring.close()
    mask = mask_ref[...].reshape(n * ns, res)
    pick = (lax.broadcasted_iota(jnp.int32, (rows, res), 1) ==
            lax.broadcasted_iota(jnp.int32, (rows, res), 0) + me * rows).astype(BF16)
    pairs = dot(dot_t(pick, mask).astype(BF16), mask)
    ninv = 1.0 / (pairs + 1e-3)
    for i in range(rows):
        ninv_ref[i] = ninv[i:i + 1]
    cnt_ref[...] = dot(jnp.ones((8, n * ns), BF16), mask)[0:1]
    for ib in range(nblk):
        ring(ib).close()


def row_kernel(heads, hd, scale, e_ref, m_ref, packed_ref, win_ref, bg_ref, wout_ref, cin_ref,
               e1_ref, g_ref, kv_ref, qsum_ref,
               rhs_ref, kaug_ref, va_ref, att_ref, bias_ref, xn_ref, wt_ref, ot_ref, ct_ref, gb_ref, top_ref):
    us, ch, res = e_ref.shape
    ht = heads * hd
    wide = us * res
    step = pl.program_id(0)

    @pl.when(step == 0)
    def _():
        rows = lax.broadcasted_iota(jnp.int32, rhs_ref.shape, 1)
        rhs_ref[...] = jnp.where(rows == 2 * ht, 1.0, 0.0).astype(BF16)
        qsum_ref[...] = jnp.zeros_like(qsum_ref)
        wt_ref[...] = flip(win_ref[...])
        ot_ref[...] = flip(wout_ref[...])
        ct = flip(cin_ref[...])
        r = lax.broadcasted_iota(jnp.int32, (ht, ht), 0)
        turn = (lax.broadcasted_iota(jnp.int32, (ht, ht), 1) == lax.rem(r, heads) * hd + r // heads).astype(BF16)
        ct_ref[...] = jnp.concatenate([dot(turn, ct[:ht]).astype(BF16), ct[ht:]], axis=0)
        gb_ref[...] = column(bg_ref[...])
        for h in range(heads):
            one = jnp.concatenate([packed_ref[d, t, h] for d in range(packed_ref.shape[0])
                                   for t in range(packed_ref.shape[1])], axis=0)
            bias_ref[h // 2, :, (h % 2) * res:(h % 2 + 1) * res] = jnp.transpose(one.astype(F32)) * LOG2E
        top = jnp.abs(bias_ref[0])
        for pr in range(1, heads // 2):
            top = jnp.maximum(top, jnp.abs(bias_ref[pr]))
        top_ref[0] = wide_max(top)

    def source():
        return jnp.concatenate([e_ref[u] for u in range(us)], axis=1).astype(F32)

    def project(n):
        return dot(wt_ref[n * ht:(n + 1) * ht], xn_ref[...]).astype(BF16)

    xn_ref[...] = norm_rows(source())
    keep = mask_row(m_ref, step * us, us)
    qs = project(0).astype(F32) * (scale * LOG2E)
    k = project(1)
    v = project(2).astype(F32)
    per_head = (lax.broadcasted_iota(jnp.int32, (heads, ht), 1) // hd ==
                lax.broadcasted_iota(jnp.int32, (heads, ht), 0)).astype(BF16)
    q_top = wide_max(dot(per_head, (qs * qs).astype(BF16)))
    k_top = wide_max(dot(per_head, k * k))
    small = (q_top * k_top < 880.0) & (top_ref[0] < 30.0) & (wide_max(jnp.abs(v)) < 1e15)

    first_half = (lax.broadcasted_iota(jnp.int32, (ht, wide), 0) % 16) < 8
    hi = qs.astype(BF16).astype(F32)
    for n, part in enumerate((hi, qs - hi)):
        even = jnp.where(first_half, part, 0.0).astype(BF16)
        odd = jnp.where(first_half, 0.0, part).astype(BF16)
        for u in range(us):
            for h in range(heads):
                rows = slice(16 * (h // 2), 16 * (h // 2) + 16)
                rhs_ref[u, n * ht + rows.start:n * ht + rows.stop, h * res:(h + 1) * res] = \
                    (odd if h % 2 else even)[rows, u * res:(u + 1) * res]
    pen = jnp.where(lax.broadcasted_iota(jnp.int32, (16, wide), 0) == 0,
                    jnp.broadcast_to(jnp.where(keep > 0, 0.0, -1e30), (16, wide)), 0.0)
    kaug_ref[...] = jnp.transpose(jnp.concatenate([k, k, pen.astype(BF16)], axis=0))
    ones = jnp.where(lax.broadcasted_iota(jnp.int32, (8, wide), 0) == 0, 1.0, 0.0)
    for pr in range(heads // 2):
        va_ref[pr] = jnp.concatenate([v[16 * pr:16 * pr + 8], ones, v[16 * pr + 8:16 * pr + 16], ones], axis=0).astype(BF16)

    @pl.when(small)
    def _():
        for u in range(us):
            cols = slice(u * res, (u + 1) * res)
            for pr in range(heads // 2):
                s = dot(kaug_ref[cols], rhs_ref[u, :, 2 * pr * res:(2 * pr + 2) * res]) + bias_ref[pr]
                o = dot(va_ref[pr, :, cols], jnp.exp2(s).astype(BF16))
                att_ref[16 * pr:16 * pr + 8, cols] = o[0:8, :res] / o[8:9, :res]
                att_ref[16 * pr + 8:16 * pr + 16, cols] = o[16:24, res:] / o[24:25, res:]
            some = jnp.max(keep[:, cols], axis=1, keepdims=True) > 0
            flat = jnp.mean(v[:, cols], axis=1, keepdims=True)
            att_ref[:, cols] = jnp.where(some, att_ref[:, cols], flat)

    @pl.when(jnp.logical_not(small))
    def _():
        def one(t, _):
            u, pr = t // (heads // 2), t % (heads // 2)
            cols = pl.ds(pl.multiple_of(u * res, res), res)
            s = dot(kaug_ref[cols], rhs_ref[u, :, pl.ds(pl.multiple_of(2 * pr * res, 2 * res), 2 * res)]) + bias_ref[pr]
            p = jnp.exp2(s - jnp.max(s, axis=0, keepdims=True)).astype(BF16)
            o = dot(va_ref[pr, :, cols], p)
            att_ref[pl.ds(pl.multiple_of(16 * pr, 16), 8), cols] = o[0:8, :res] / o[8:9, :res]
            att_ref[pl.ds(pl.multiple_of(16 * pr + 8, 8), 8), cols] = o[16:24, res:] / o[24:25, res:]
            return 0

        lax.fori_loop(0, us * (heads // 2), one, 0)

    gated = (sigmoid(project(3).astype(F32) + gb_ref[...]) * att_ref[...]).astype(BF16)
    e1 = (source() + dot(ot_ref[...], gated)).astype(BF16)
    e1_ref[0] = e1
    col = dot(ct_ref[...], norm_rows(e1.astype(F32))).astype(BF16)
    part = col[:ht].astype(F32) * keep
    tot = part[:, :res]
    for u in range(1, us):
        tot = tot + part[:, u * res:(u + 1) * res]
    qsum_ref[...] += tot
    g_ref[0] = col[ht:2 * ht]
    kv_ref[0] = col[2 * ht:]


def exchange(axis, me, n, srcs, dst, send_sem, recv_sem):
    copies = []
    for t in range(1, n):
        peer = lax.rem(me + t, n)
        copy = pltpu.make_async_remote_copy(src_ref=srcs(peer), dst_ref=dst.at[me], send_sem=send_sem.at[t],
                                            recv_sem=recv_sem.at[t], device_id={axis: peer}, device_id_type=MESH)
        copy.start()
        copies.append(copy)
    return copies


def column_attention(axis, n, heads, hd, scale, qsum_ref, cnt_ref, kv_ref, m_ref, o_ref,
                     l_ref, qp_ref, qb_ref, st_ref, sp_ref, send_sem, recv_sem):
    ng, _, wide = kv_ref.shape
    res = qsum_ref.shape[1]
    us = wide // res
    ht = heads * hd
    me = lax.axis_index(axis)
    blk = ht // n
    mine = pl.ds(pl.multiple_of(me * blk, blk), blk)
    copies = exchange(axis, me, n, lambda p: qsum_ref.at[pl.ds(pl.multiple_of(p * blk, blk), blk)], qp_ref,
                      send_sem.at[0], recv_sem.at[0])
    qp_ref[me] = qsum_ref[mine]
    for c in copies:
        c.wait()
    tot = qp_ref[0]
    for t in range(1, n):
        tot = tot + qp_ref[t]
    qb_ref[me] = (tot / (cnt_ref[...] + 1e-10)).astype(BF16).astype(F32)
    copies = exchange(axis, me, n, lambda p: qb_ref.at[me], qb_ref, send_sem.at[1], recv_sem.at[1])
    for c in copies:
        c.wait()
    qbar = qb_ref[...].reshape(ht, res)

    def logits(gr, top):
        for u in range(us):
            cols = slice(u * res, (u + 1) * res)
            kv = kv_ref[gr, :, cols].astype(F32)
            acc = qbar[0:heads] * kv[0:1]
            for d in range(1, hd):
                acc = acc + qbar[d * heads:(d + 1) * heads] * kv[d:d + 1]
            acc = jnp.where(m_ref[pl.ds(gr * us + u, 1), :] > 0, acc * scale, MASK_FILL)
            l_ref[gr, :, cols] = acc
            top = jnp.maximum(top, acc)
        return top

    top = lax.fori_loop(0, ng, logits, jnp.full((heads, res), -3e38, F32))

    def sums(gr, carry):
        for u in range(us):
            cols = slice(u * res, (u + 1) * res)
            w = jnp.exp(l_ref[gr, :, cols] - top)
            kv = kv_ref[gr, :, cols].astype(F32)
            carry = (carry[0] + w,) + tuple(carry[1 + d] + w * kv[hd + d:hd + d + 1] for d in range(hd))
        return carry

    zero = jnp.zeros((heads, res), F32)
    tot = lax.fori_loop(0, ng, sums, (zero,) * (hd + 1))
    for d in range(hd):
        st_ref[:, d, :] = tot[1 + d]
    st_ref[:, hd, :] = tot[0]
    st_ref[:, hd + 1, :] = top
    for d in range(hd + 2, st_ref.shape[1]):
        st_ref[:, d, :] = zero
    copies = exchange(axis, me, n, lambda p: st_ref.at[p], sp_ref, send_sem.at[2], recv_sem.at[2])
    sp_ref[me] = st_ref[me]
    for c in copies:
        c.wait()
    best = sp_ref[0, hd + 1:hd + 2]
    for t in range(1, n):
        best = jnp.maximum(best, sp_ref[t, hd + 1:hd + 2])
    num = jnp.zeros((hd, res), F32)
    den = jnp.zeros((1, res), F32)
    for t in range(n):
        fac = jnp.exp(sp_ref[t, hd + 1:hd + 2] - best)
        num = num + sp_ref[t, 0:hd] * fac
        den = den + sp_ref[t, hd:hd + 1] * fac
    o_ref[me] = num / den
    copies = exchange(axis, me, n, lambda p: o_ref.at[me], o_ref, send_sem.at[3], recv_sem.at[3])
    for c in copies:
        c.wait()


def tail_kernel(axis, n, heads, hd, scale, qsum_ref, cnt_ref, kv_ref, e1_hbm, g_hbm, m_ref, bg_ref, wout_ref, tin_ref, tout_ref, opm_ref,
                z_hbm, ninv_ref, w_ref, bo_ref, e3_hbm, out_hbm,
                o_ref, l_ref, qp_ref, qb_ref, st_ref, sp_ref, csend, crecv, e1_ref, g_ref, e3_ref, z_ref, buf_ref, a_ref, b_ref, ag_ref, tr_ref, bg_all, at_ref, hi_ref, lo_ref,
                wp_ref, wf_ref, local, asend, arecv, bsend, brecv):
    rows, res, pd = z_ref.shape
    nb, odim, ns, jb = b_ref.shape
    chips = a_ref.shape[0]
    ht = heads * hd
    wide = e1_ref.shape[2]
    us = wide // res
    tb = buf_ref.shape[1]
    ngr = ns // tb
    per = tb // us
    ib = 2 * hi_ref.shape[0]
    half = odim // 2
    me = lax.axis_index(axis)
    chip, core = me // 2, lax.rem(me, 2)
    right, left, far, other = neighbours(me, n)
    up, down, across = lax.rem(chip + 1, chips), lax.rem(chip + chips - 1, chips), lax.rem(chip + 2, chips)

    def fetch(g):
        at = pl.ds(g * per, per)
        return [pltpu.make_async_copy(e1_hbm.at[at], e1_ref.at[at], local.at[0, g]),
                pltpu.make_async_copy(g_hbm.at[at], g_ref.at[at], local.at[1, g])]

    for g in range(ngr):
        for c in fetch(g):
            c.start()
    z_in = pltpu.make_async_copy(z_hbm, z_ref, local.at[2, 0])
    z_in.start()
    enter(axis, me, n)

    part = {None: slice(None), 0: pl.ds(0, half), 1: pl.ds(half, half)}

    def a_copies(g):
        seqs = pl.ds(pl.multiple_of(g * tb, tb), tb)
        src = lambda c, p=None: a_ref.at[c, part[p], seqs]
        dst = lambda d, p=None: ag_ref.at[d, part[p], seqs]
        tr = lambda t: tr_ref.at[t, :, seqs]
        plan = [(src(across, 0), tr(0), right), (src(across, 1), tr(1), left), (src(up), dst(me), right),
                (src(down), dst(me), left), (src(chip), dst(me), other),
                (tr(0), dst(left, 0), right), (tr(1), dst(right, 1), left),
                (dst(left), dst(left), other), (dst(right), dst(right), other),
                (dst(far, 0), dst(far, 0), other), (dst(far, 1), dst(far, 1), other)]
        return lambda k: remote(axis, (asend.at[g, k], arecv.at[g, k]), *plan[k])

    def b_first(g):
        seqs = pl.ds(pl.multiple_of(g * tb, tb), tb)
        return Gather(axis, me, n, lambda k: (bsend.at[g, k], brecv.at[g, k]), b_ref.at[0, :, seqs],
                      lambda d, p=None: bg_all.at[0, d, part[p], seqs])

    def b_rest(t):
        return Gather(axis, me, n, lambda k: (bsend.at[ngr - 1 + t, k], brecv.at[ngr - 1 + t, k]), b_ref.at[t],
                      lambda d, p=None: bg_all.at[t, d] if p is None else bg_all.at[t, d, part[p]])

    src = lax.broadcasted_iota(jnp.int32, (res, chips * jb), 0)
    dst = lax.broadcasted_iota(jnp.int32, (res, chips * jb), 1)
    hj = jb // 2
    place = ((dst % hj < rows) & (src == (dst // hj) * rows + dst % hj)).astype(BF16)

    wout, tin, opm = (flip(r[...]) for r in (wout_ref, tin_ref, opm_ref))
    gate_bias = column(bg_ref[...])
    column_attention(axis, n, heads, hd, scale, qsum_ref, cnt_ref, kv_ref, m_ref, o_ref,
                     l_ref, qp_ref, qb_ref, st_ref, sp_ref, csend, crecv)

    def group(g, _):
        seqs = pl.ds(pl.multiple_of(g * tb, tb), tb)
        for c in fetch(g):
            c.wait()
        o = jnp.concatenate([o_ref[...].reshape(ht, res)] * us, axis=1)
        for j in range(per):
            gr = g * per + j
            gated = (sigmoid(g_ref[gr].astype(F32) + gate_bias) * o).astype(BF16)
            e2 = (e1_ref[gr].astype(F32) + dot(wout, gated)).astype(BF16).astype(F32)
            hid = jnp.maximum(dot(tin, norm_rows(e2)), 0.0).astype(BF16)
            e3 = (e2 + dot(tout_ref[...], hid)).astype(BF16)
            ab = dot(opm, norm_rows(e3.astype(F32))).astype(BF16).astype(F32) * mask_row(m_ref, gr * us, us)
            for u in range(us):
                cols = slice(u * res, (u + 1) * res)
                e3_ref[gr * us + u] = e3[:, cols]
                buf_ref[:, j * us + u, :] = ab[:, cols]
        moved = dot(buf_ref[0:odim].astype(BF16).reshape(odim * tb, res), place).astype(BF16)
        for c in range(chips):
            a_ref[c, :, seqs, :] = moved[:, c * jb:(c + 1) * jb].reshape(odim, tb, jb)
        for t in range(nb):
            blk = buf_ref[odim:, :, t * jb:(t + 1) * jb].astype(BF16)
            b_ref[t, :, seqs, :] = blk
            bg_all[t, me, :, seqs, :] = blk
        ac = a_copies(g)
        for k in range(5):
            ac(k).start()
        b_first(g).open()
        ag_ref[me, :, seqs, :] = a_ref[chip, :, seqs, :]
        return 0

    lax.fori_loop(0, ngr, group, 0)
    e3_out = pltpu.make_async_copy(e3_ref, e3_hbm, local.at[2, 1])
    e3_out.start()

    def pass_on(g, _):
        ac = a_copies(g)
        for wait, start in ((0, 5), (1, 6), (2, 7), (3, 8)):
            ac(wait).wait_recv()
            ac(start).start()
        b_first(g).hand_on()
        return 0

    lax.fori_loop(0, ngr, pass_on, 0)
    b_rest(1).open()

    def finish_a(g, _):
        ac = a_copies(g)
        for wait, start in ((5, 9), (6, 10)):
            ac(wait).wait_recv()
            ac(start).start()
        for k in (4, 7, 8, 9, 10):
            ac(k).wait_recv()
        for k in range(11):
            ac(k).wait_send()
        return 0

    lax.fori_loop(0, ngr, finish_a, 0)
    wf_ref[...] = w_ref[...].astype(F32)
    for d in range(odim):
        wp_ref[:, d * odim:(d + 1) * odim] = jnp.transpose(wf_ref[:, d, :]).astype(BF16)
    pick = (lax.broadcasted_iota(jnp.int32, (rows, jb), 1) ==
            lax.broadcasted_iota(jnp.int32, (rows, jb), 0) + core * hj).astype(BF16)
    for c in range(odim):
        at_ref[:, c, :] = dot_t(pick, ag_ref[:, c].reshape(n * ns, jb))

    def finish_b(g, _):
        b_first(g).close()
        return 0

    lax.fori_loop(0, ngr, finish_b, 0)
    z_in.wait()
    steps = rows // ib

    def done(t):
        at = pl.ds(t * jb, jb)
        return pltpu.make_async_copy(z_ref.at[:, at], out_hbm.at[:, at], local.at[3, t])

    def body(k, _):
        t = k // steps
        base = lax.rem(k, steps) * ib
        cols = pl.ds(pl.multiple_of(t * jb, jb), jb)

        for later in range(1, nb):
            @pl.when(k == (later - 1) * steps + steps // 2)
            def _():
                b_rest(later).hand_on()
                if later + 1 < nb:
                    b_rest(later + 1).open()

            @pl.when(k == later * steps)
            def _():
                b_rest(later).close()
                done(later - 1).start()

        a = at_ref[pl.ds(base, ib)].reshape(ib * odim, n * ns).astype(BF16)
        for q in range(odim // 2):
            rhs = jnp.concatenate([bg_all[t, :, 2 * q].reshape(n * ns, jb), bg_all[t, :, 2 * q + 1].reshape(n * ns, jb)], axis=1)
            pr = dot(a, rhs)
            hi = pr.astype(BF16)
            lo = (pr - hi.astype(F32)).astype(BF16)
            for val, ref in ((hi, hi_ref), (lo, lo_ref)):
                for i in range(ib):
                    for h in range(2):
                        ref[i // 2, (2 * q + h) * odim:(2 * q + h + 1) * odim, (i % 2) * jb:(i % 2 + 1) * jb] = \
                            val[i * odim:(i + 1) * odim, h * jb:(h + 1) * jb]
        for ip in range(ib // 2):
            zt = dot(wp_ref[...], hi_ref[ip]) + dot(wp_ref[...], lo_ref[ip])
            for h in range(2):
                i = base + 2 * ip + h
                upd = jnp.transpose(zt[:, h * jb:(h + 1) * jb] * ninv_ref[i, :, cols])
                z_ref[i, cols, :] = (z_ref[i, cols, :].astype(F32) + upd + bo_ref[...].astype(F32)).astype(BF16)
        return 0

    lax.fori_loop(0, nb * steps, body, 0)
    done(nb - 1).start()
    for t in range(nb):
        done(t).wait()
    e3_out.wait()


def solution(mesh):
    row_spec = P(('batch', 'seq'))
    rep_spec = P()
    n_seq = mesh.shape['seq']

    def local_block(msa, mask, pair, w_pair_bias, w_row_in, b_row_gate, w_row_out, w_col_in, b_col_gate, w_col_out,
                    w_trans_in, w_trans_out, w_opm_in, w_opm_out, b_opm_out):
        ns, res, ch = msa.shape
        rows = pair.shape[0]
        pd = pair.shape[-1]
        heads = w_pair_bias.shape[1]
        ht = w_row_out.shape[0]
        hd = ht // heads
        odim = w_opm_out.shape[0]
        scale = hd ** -0.5
        params = functools.partial(pltpu.CompilerParams, vmem_limit_bytes=VMEM_LIMIT)

        vm = pl.BlockSpec(memory_space=pltpu.VMEM)
        hbm = pl.BlockSpec(memory_space=pl.ANY)
        dma = pltpu.SemaphoreType.DMA
        tall = 16
        nblk = rows // tall
        packed, _, ninv, counts = pl.pallas_call(
            functools.partial(bias_kernel, 'seq', n_seq),
            in_specs=[hbm, vm, vm],
            out_specs=[vm] * 4,
            out_shape=[jax.ShapeDtypeStruct((n_seq, nblk, heads, tall, res), BF16), jax.ShapeDtypeStruct((n_seq, ns, res), BF16),
                       jax.ShapeDtypeStruct((rows, 1, res), F32), jax.ShapeDtypeStruct((1, res), F32)],
            scratch_shapes=[pltpu.VMEM((rows, res, pd), BF16), pltpu.VMEM((heads, tall, res), F32), dma((nblk,)),
                            dma((nblk + 1, 9)), dma((nblk + 1, 9))],
            compiler_params=params(collective_id=1, has_side_effects=True),
            name='pair_bias',
        )(pair, w_pair_bias.T, mask)

        us = SEQS
        ng, wide = ns // us, us * res
        ncol = w_col_in.shape[1]

        full = lambda *shape: pl.BlockSpec(shape, lambda *g: (0,) * len(shape))
        group = lambda k, r: pl.BlockSpec((k, r, wide), lambda s: (s, 0, 0))
        e1, gate, kv, qsum = pl.pallas_call(
            functools.partial(row_kernel, heads, hd, scale),
            grid=(ng,),
            in_specs=[pl.BlockSpec((us, ch, res), lambda s: (s, 0, 0)), full(ns, res),
                      full(n_seq, nblk, heads, tall, res), full(ch, 4 * ht), full(1, ht), full(ht, ch), full(ch, ncol)],
            out_specs=[group(1, ch), group(1, ht), group(1, 2 * hd), full(ht, res)],
            out_shape=[jax.ShapeDtypeStruct((ng, ch, wide), BF16), jax.ShapeDtypeStruct((ng, ht, wide), BF16),
                       jax.ShapeDtypeStruct((ng, 2 * hd, wide), BF16), jax.ShapeDtypeStruct((ht, res), F32)],
            scratch_shapes=[pltpu.VMEM((us, 2 * ht + 16, heads * res), BF16), pltpu.VMEM((wide, 2 * ht + 16), BF16),
                            pltpu.VMEM((heads // 2, 32, wide), BF16), pltpu.VMEM((ht, wide), F32),
                            pltpu.VMEM((heads // 2, res, 2 * res), F32), pltpu.VMEM((ch, wide), BF16), pltpu.VMEM((4 * ht, ch), BF16),
                            pltpu.VMEM((ch, ht), BF16), pltpu.VMEM((ncol, ch), BF16), pltpu.VMEM((ht, 1), F32), pltpu.SMEM((1,), F32)],
            compiler_params=params(dimension_semantics=('arbitrary',)),
            name='row_attention',
        )(jnp.transpose(msa, (0, 2, 1)), mask, packed, w_row_in, b_row_gate.reshape(1, ht), w_row_out, w_col_in)

        tb, jb, ib = 16, 128, 8
        chips = n_seq // 2
        nb = res // jb
        e3, pair_out = pl.pallas_call(
            functools.partial(tail_kernel, 'seq', n_seq, heads, hd, scale),
            in_specs=[vm] * 3 + [hbm] * 2 + [vm] * 6 + [hbm] + [vm] * 3,
            out_specs=[hbm, hbm],
            out_shape=[jax.ShapeDtypeStruct((ns, ch, res), BF16), jax.ShapeDtypeStruct((rows, res, pd), BF16)],
            scratch_shapes=[pltpu.VMEM((heads, hd, res), F32), pltpu.VMEM((ng, heads, wide), F32),
                            pltpu.VMEM((n_seq, ht // n_seq, res), F32), pltpu.VMEM((n_seq, ht // n_seq, res), F32),
                            pltpu.VMEM((heads, 16, res), F32), pltpu.VMEM((n_seq, 16, res), F32), dma((4, n_seq)), dma((4, n_seq)),
                            pltpu.VMEM((ng, ch, wide), BF16), pltpu.VMEM((ng, ht, wide), BF16), pltpu.VMEM((ns, ch, res), BF16),
                            pltpu.VMEM((rows, res, pd), BF16), pltpu.VMEM((2 * odim, tb, res), F32),
                            pltpu.VMEM((chips, odim, ns, jb), BF16), pltpu.VMEM((nb, odim, ns, jb), BF16),
                            pltpu.VMEM((n_seq, odim, ns, jb), BF16), pltpu.VMEM((2, odim // 2, ns, jb), BF16),
                            pltpu.VMEM((nb, n_seq, odim, ns, jb), BF16), pltpu.VMEM((rows, odim, n_seq * ns), F32),
                            pltpu.VMEM((ib // 2, odim * odim, 2 * jb), BF16), pltpu.VMEM((ib // 2, odim * odim, 2 * jb), BF16),
                            pltpu.VMEM((pd, odim * odim), BF16), pltpu.VMEM((odim, odim, pd), F32),
                            dma((4, max(4, ns // tb))), dma((ns // tb, 11)), dma((ns // tb, 11)),
                            dma((ns // tb + nb - 1, 9)), dma((ns // tb + nb - 1, 9))],
            compiler_params=params(collective_id=2, has_side_effects=True),
            name='tail_outer_product',
        )(qsum, counts, kv, e1, gate, mask, b_col_gate.reshape(1, ht), w_col_out, w_trans_in, w_trans_out.T, w_opm_in,
          pair, ninv, w_opm_out, b_opm_out.reshape(1, pd))
        return jnp.transpose(e3, (0, 2, 1)), pair_out

    return jax.shard_map(local_block, mesh=mesh, in_specs=(row_spec, row_spec, row_spec) + (rep_spec,) * 12,
                         out_specs=(row_spec, row_spec), check_vma=False)
```

```python
import functools
import math

import jax
import jax.numpy as jnp
from jax import lax
from jax.experimental import pallas as pl
from jax.experimental.pallas import tpu as pltpu
from jax.sharding import PartitionSpec as P

MASK_FILL = -1e9
LOG2E = math.log2(math.e)
F32 = jnp.float32
BF16 = jnp.bfloat16
VMEM_LIMIT = 62 * 1024 * 1024
MESH = pl.DeviceIdType.MESH
SEQS = 8
GROUP = 4


def norm_rows(x):
    c = x - jnp.mean(x, axis=0, keepdims=True)
    var = jnp.mean(c * c, axis=0, keepdims=True)
    return (c * lax.rsqrt(var + 1e-5)).astype(BF16)


def dot(a, b):
    return jnp.dot(a, b, preferred_element_type=F32)


def dot_t(a, b):
    return lax.dot_general(a, b, (((1,), (1,)), ((), ())), preferred_element_type=F32)


def sigmoid(x):
    return 1.0 / (1.0 + jnp.exp(-x))


def wide_max(x):
    return jnp.max(jnp.max(x, axis=0, keepdims=True), axis=1, keepdims=True)[0, 0]


def enter(axis, me, n):
    barrier = pltpu.get_barrier_semaphore()
    for t in range(1, n):
        pl.semaphore_signal(barrier, inc=1, device_id={axis: lax.rem(me + t, n)}, device_id_type=MESH)
    pl.semaphore_wait(barrier, n - 1)


def neighbours(me, n):
    return lax.rem(me + 2, n), lax.rem(me + n - 2, n), lax.rem(me + 4, n), me + 1 - 2 * lax.rem(me, 2)


def remote(axis, sems, src, dst, to):
    return pltpu.make_async_remote_copy(src_ref=src, dst_ref=dst, send_sem=sems[0], recv_sem=sems[1],
                                        device_id={axis: to}, device_id_type=MESH)


class Gather:
    def __init__(self, axis, me, n, sems, own, view):
        right, left, far, other = neighbours(me, n)
        plan = [(own, view(me), right), (own, view(me), left), (own, view(me), other),
                (view(left, 0), view(left, 0), right), (view(right, 1), view(right, 1), left),
                (view(left), view(left), other), (view(right), view(right), other),
                (view(far, 0), view(far, 0), other), (view(far, 1), view(far, 1), other)]
        self.copy = lambda k: remote(axis, sems(k), *plan[k])

    def after(self, waits, starts):
        for k in waits:
            self.copy(k).wait_recv()
        for k in starts:
            self.copy(k).start()

    def open(self):
        self.after((), (0, 1, 2))

    def hand_on(self):
        self.after((0,), (3, 5))
        self.after((1,), (4, 6))

    def close(self):
        self.after((3,), (7,))
        self.after((4,), (8,))
        self.after((2, 5, 6, 7, 8), ())
        for k in range(9):
            self.copy(k).wait_send()


def identity(size):
    return (lax.broadcasted_iota(jnp.int32, (size, size), 0) == lax.broadcasted_iota(jnp.int32, (size, size), 1)).astype(BF16)


def flip(x):
    return jnp.transpose(x.astype(F32)).astype(BF16)


def column(row):
    k = row.shape[1]
    on = lax.broadcasted_iota(jnp.int32, (k, k), 0) == lax.broadcasted_iota(jnp.int32, (k, k), 1)
    return jnp.sum(jnp.where(on, jnp.broadcast_to(row.astype(F32), (k, k)), 0.0), axis=1, keepdims=True)


def mask_row(m_ref, first, count):
    return jnp.concatenate([m_ref[pl.ds(first + u, 1), :] for u in range(count)], axis=1).astype(F32)


def bias_kernel(axis, n, z_hbm, w_ref, m_ref, out_ref, mask_ref, ninv_ref, cnt_ref, z_ref, blk_ref, local, send_sem, recv_sem):
    rows, res, pd = z_ref.shape
    heads = w_ref.shape[0]
    nblk, tall = out_ref.shape[1], out_ref.shape[3]
    ns = m_ref.shape[0]
    step = 4
    me = lax.axis_index(axis)

    def fetch(ib):
        at = pl.ds(ib * tall, tall)
        return pltpu.make_async_copy(z_hbm.at[at], z_ref.at[at], local.at[ib])

    for ib in range(nblk):
        fetch(ib).start()
    mask_ref[me] = m_ref[...].astype(BF16)
    enter(axis, me, n)
    hh, hs = heads // 2, ns // 2
    sems = lambda t: lambda k: (send_sem.at[t, k], recv_sem.at[t, k])
    mask_ring = Gather(axis, me, n, sems(nblk), mask_ref.at[me],
                       lambda d, p=None: mask_ref.at[d] if p is None else mask_ref.at[d, pl.ds(p * hs, hs)])

    def ring(ib):
        return Gather(axis, me, n, sems(ib), out_ref.at[me, ib],
                      lambda d, p=None: out_ref.at[d, ib] if p is None else out_ref.at[d, ib, pl.ds(p * hh, hh)])

    mask_ring.open()
    eye = identity(pd)

    def block(ib, _):
        fetch(ib).wait()
        for t in range(tall // step):
            zt = dot_t(eye, z_ref[pl.ds(ib * tall + t * step, step)].reshape(step * res, pd))
            b = dot(w_ref[...], norm_rows(zt))
            for u in range(step):
                blk_ref[:, t * step + u, :] = b[:, u * res:(u + 1) * res]
        out_ref[me, ib] = blk_ref[...].astype(BF16)
        ring(ib).open()
        return 0

    lax.fori_loop(0, nblk, block, 0)
    mask_ring.hand_on()
    for ib in range(nblk):
        ring(ib).hand_on()
    mask_ring.close()
    mask = mask_ref[...].reshape(n * ns, res)
    pick = (lax.broadcasted_iota(jnp.int32, (rows, res), 1) ==
            lax.broadcasted_iota(jnp.int32, (rows, res), 0) + me * rows).astype(BF16)
    pairs = dot(dot_t(pick, mask).astype(BF16), mask)
    ninv = 1.0 / (pairs + 1e-3)
    for i in range(rows):
        ninv_ref[i] = ninv[i:i + 1]
    cnt_ref[...] = dot(jnp.ones((8, n * ns), BF16), mask)[0:1]
    for ib in range(nblk):
        ring(ib).close()


def row_kernel(heads, hd, scale, e_ref, m_ref, packed_ref, win_ref, bg_ref, wout_ref, cin_ref,
               e1_ref, g_ref, kv_ref, qsum_ref,
               rhs_ref, kaug_ref, v_ref, att_ref, bias_ref, xn_ref, wt_ref, ot_ref, ct_ref, gb_ref, top_ref):
    us, ch, res = e_ref.shape
    ht = heads * hd
    wide = us * res
    step = pl.program_id(0)

    @pl.when(step == 0)
    def _():
        rows = lax.broadcasted_iota(jnp.int32, rhs_ref.shape, 1)
        rhs_ref[...] = jnp.where(rows == 2 * GROUP * hd, 1.0, 0.0).astype(BF16)
        qsum_ref[...] = jnp.zeros_like(qsum_ref)
        wt_ref[...] = flip(win_ref[...])
        ot_ref[...] = flip(wout_ref[...])
        ct = flip(cin_ref[...])
        r = lax.broadcasted_iota(jnp.int32, (ht, ht), 0)
        turn = (lax.broadcasted_iota(jnp.int32, (ht, ht), 1) == lax.rem(r, heads) * hd + r // heads).astype(BF16)
        ct_ref[...] = jnp.concatenate([dot(turn, ct[:ht]).astype(BF16), ct[ht:]], axis=0)
        gb_ref[...] = column(bg_ref[...])
        for h in range(heads):
            one = jnp.concatenate([packed_ref[d, t, h] for d in range(packed_ref.shape[0])
                                   for t in range(packed_ref.shape[1])], axis=0)
            bias_ref[h // GROUP, :, (h % GROUP) * res:(h % GROUP + 1) * res] = jnp.transpose(one.astype(F32)) * LOG2E
        top = jnp.abs(bias_ref[0])
        for gr in range(1, heads // GROUP):
            top = jnp.maximum(top, jnp.abs(bias_ref[gr]))
        top_ref[0] = wide_max(top)

    def source():
        return jnp.concatenate([e_ref[u] for u in range(us)], axis=1).astype(F32)

    def project(n):
        return dot(wt_ref[n * ht:(n + 1) * ht], xn_ref[...]).astype(BF16)

    xn_ref[...] = norm_rows(source())
    keep = mask_row(m_ref, step * us, us)
    qs = project(0).astype(F32) * (scale * LOG2E)
    k = project(1)
    v = project(2).astype(F32)
    per_head = (lax.broadcasted_iota(jnp.int32, (heads, ht), 1) // hd ==
                lax.broadcasted_iota(jnp.int32, (heads, ht), 0)).astype(BF16)
    q_top = wide_max(dot(per_head, (qs * qs).astype(BF16)))
    k_top = wide_max(dot(per_head, k * k))
    small = (q_top * k_top < 880.0) & (top_ref[0] < 30.0) & (wide_max(jnp.abs(v)) < 1e15)

    gw = GROUP * hd
    row_head = (lax.broadcasted_iota(jnp.int32, (ht, wide), 0) // hd) % GROUP
    hi = qs.astype(BF16).astype(F32)
    for n, part in enumerate((hi, qs - hi)):
        for r in range(GROUP):
            only = jnp.where(row_head == r, part, 0.0).astype(BF16)
            for u in range(us):
                for h in range(r, heads, GROUP):
                    rhs_ref[u, gw * n:gw * (n + 1), h * res:(h + 1) * res] = \
                        only[gw * (h // GROUP):gw * (h // GROUP + 1), u * res:(u + 1) * res]
    pen = jnp.where(lax.broadcasted_iota(jnp.int32, (16, wide), 0) == 0,
                    jnp.broadcast_to(jnp.where(keep > 0, 0.0, -1e30), (16, wide)), 0.0)
    for gr in range(heads // GROUP):
        kp = k[gw * gr:gw * (gr + 1)]
        kaug_ref[gr] = jnp.transpose(jnp.concatenate([kp, kp, pen.astype(BF16)], axis=0))
    v_ref[...] = v.astype(BF16)

    def attend(cols, gr, rows, lanes, at_row, shifted):
        s = dot(kaug_ref[gr, cols], lanes) + bias_ref[gr]
        p = jnp.exp2(s - jnp.max(s, axis=0, keepdims=True)) if shifted else jnp.exp2(s)
        den = jnp.sum(p, axis=0, keepdims=True)
        o = dot(v_ref[rows, cols], p.astype(BF16))
        for r in range(GROUP):
            att_ref[at_row(r), cols] = o[hd * r:hd * (r + 1), r * res:(r + 1) * res] / den[:, r * res:(r + 1) * res]

    @pl.when(small)
    def _():
        for u in range(us):
            cols = slice(u * res, (u + 1) * res)
            for gr in range(heads // GROUP):
                attend(cols, gr, slice(gw * gr, gw * (gr + 1)), rhs_ref[u, :, gr * GROUP * res:(gr + 1) * GROUP * res],
                       lambda r: slice(gw * gr + hd * r, gw * gr + hd * (r + 1)), False)
            some = jnp.max(keep[:, cols], axis=1, keepdims=True) > 0
            flat = jnp.mean(v[:, cols], axis=1, keepdims=True)
            att_ref[:, cols] = jnp.where(some, att_ref[:, cols], flat)

    @pl.when(jnp.logical_not(small))
    def _():
        def one(t, _):
            u, gr = t // (heads // GROUP), t % (heads // GROUP)
            cols = pl.ds(pl.multiple_of(u * res, res), res)
            attend(cols, gr, pl.ds(pl.multiple_of(gw * gr, gw), gw),
                   rhs_ref[u, :, pl.ds(pl.multiple_of(gr * GROUP * res, GROUP * res), GROUP * res)],
                   lambda r: pl.ds(pl.multiple_of(gw * gr + hd * r, hd), hd), True)
            return 0

        lax.fori_loop(0, us * (heads // GROUP), one, 0)

    gated = (sigmoid(project(3).astype(F32) + gb_ref[...]) * att_ref[...]).astype(BF16)
    e1 = (source() + dot(ot_ref[...], gated)).astype(BF16)
    e1_ref[0] = e1
    col = dot(ct_ref[...], norm_rows(e1.astype(F32))).astype(BF16)
    part = col[:ht].astype(F32) * keep
    tot = part[:, :res]
    for u in range(1, us):
        tot = tot + part[:, u * res:(u + 1) * res]
    qsum_ref[...] += tot
    g_ref[0] = col[ht:2 * ht]
    kv_ref[0] = col[2 * ht:]


def exchange(axis, me, n, srcs, dst, send_sem, recv_sem):
    copies = []
    for t in range(1, n):
        peer = lax.rem(me + t, n)
        copy = pltpu.make_async_remote_copy(src_ref=srcs(peer), dst_ref=dst.at[me], send_sem=send_sem.at[t],
                                            recv_sem=recv_sem.at[t], device_id={axis: peer}, device_id_type=MESH)
        copy.start()
        copies.append(copy)
    return copies


def column_attention(axis, n, heads, hd, scale, qsum_ref, cnt_ref, kv_ref, m_ref, o_ref,
                     l_ref, qp_ref, qb_ref, st_ref, sp_ref, send_sem, recv_sem):
    ng, _, wide = kv_ref.shape
    res = qsum_ref.shape[1]
    us = wide // res
    ht = heads * hd
    me = lax.axis_index(axis)
    blk = ht // n
    mine = pl.ds(pl.multiple_of(me * blk, blk), blk)
    copies = exchange(axis, me, n, lambda p: qsum_ref.at[pl.ds(pl.multiple_of(p * blk, blk), blk)], qp_ref,
                      send_sem.at[0], recv_sem.at[0])
    qp_ref[me] = qsum_ref[mine]
    for c in copies:
        c.wait()
    tot = qp_ref[0]
    for t in range(1, n):
        tot = tot + qp_ref[t]
    qb_ref[me] = (tot / (cnt_ref[...] + 1e-10)).astype(BF16).astype(F32)
    copies = exchange(axis, me, n, lambda p: qb_ref.at[me], qb_ref, send_sem.at[1], recv_sem.at[1])
    for c in copies:
        c.wait()
    qbar = qb_ref[...].reshape(ht, res)

    def logits(gr, top):
        for u in range(us):
            cols = slice(u * res, (u + 1) * res)
            kv = kv_ref[gr, :, cols].astype(F32)
            acc = qbar[0:heads] * kv[0:1]
            for d in range(1, hd):
                acc = acc + qbar[d * heads:(d + 1) * heads] * kv[d:d + 1]
            acc = jnp.where(m_ref[pl.ds(gr * us + u, 1), :] > 0, acc * scale, MASK_FILL)
            l_ref[gr, :, cols] = acc
            top = jnp.maximum(top, acc)
        return top

    top = lax.fori_loop(0, ng, logits, jnp.full((heads, res), -3e38, F32))

    def sums(gr, carry):
        for u in range(us):
            cols = slice(u * res, (u + 1) * res)
            w = jnp.exp(l_ref[gr, :, cols] - top)
            kv = kv_ref[gr, :, cols].astype(F32)
            carry = (carry[0] + w,) + tuple(carry[1 + d] + w * kv[hd + d:hd + d + 1] for d in range(hd))
        return carry

    zero = jnp.zeros((heads, res), F32)
    tot = lax.fori_loop(0, ng, sums, (zero,) * (hd + 1))
    for d in range(hd):
        st_ref[:, d, :] = tot[1 + d]
    st_ref[:, hd, :] = tot[0]
    st_ref[:, hd + 1, :] = top
    for d in range(hd + 2, st_ref.shape[1]):
        st_ref[:, d, :] = zero
    copies = exchange(axis, me, n, lambda p: st_ref.at[p], sp_ref, send_sem.at[2], recv_sem.at[2])
    sp_ref[me] = st_ref[me]
    for c in copies:
        c.wait()
    best = sp_ref[0, hd + 1:hd + 2]
    for t in range(1, n):
        best = jnp.maximum(best, sp_ref[t, hd + 1:hd + 2])
    num = jnp.zeros((hd, res), F32)
    den = jnp.zeros((1, res), F32)
    for t in range(n):
        fac = jnp.exp(sp_ref[t, hd + 1:hd + 2] - best)
        num = num + sp_ref[t, 0:hd] * fac
        den = den + sp_ref[t, hd:hd + 1] * fac
    o_ref[me] = num / den
    copies = exchange(axis, me, n, lambda p: o_ref.at[me], o_ref, send_sem.at[3], recv_sem.at[3])
    for c in copies:
        c.wait()


def tail_kernel(axis, n, heads, hd, scale, qsum_ref, cnt_ref, kv_ref, e1_hbm, g_hbm, m_ref, bg_ref, wout_ref, tin_ref, tout_ref, opm_ref,
                z_hbm, ninv_ref, w_ref, bo_ref, e3_hbm, out_hbm,
                o_ref, l_ref, qp_ref, qb_ref, st_ref, sp_ref, csend, crecv, e1_ref, g_ref, e3_ref, z_ref, buf_ref, a_ref, b_ref, ag_ref, tr_ref, bg_all, at_ref, hi_ref, lo_ref,
                wp_ref, wf_ref, local, asend, arecv, bsend, brecv):
    rows, res, pd = z_ref.shape
    nb, odim, ns, jb = b_ref.shape
    chips = a_ref.shape[0]
    ht = heads * hd
    wide = e1_ref.shape[2]
    us = wide // res
    tb = buf_ref.shape[1]
    ngr = ns // tb
    per = tb // us
    ib = 2 * hi_ref.shape[0]
    half = odim // 2
    me = lax.axis_index(axis)
    chip, core = me // 2, lax.rem(me, 2)
    right, left, far, other = neighbours(me, n)
    up, down, across = lax.rem(chip + 1, chips), lax.rem(chip + chips - 1, chips), lax.rem(chip + 2, chips)

    def fetch(g):
        at = pl.ds(g * per, per)
        return [pltpu.make_async_copy(e1_hbm.at[at], e1_ref.at[at], local.at[0, g]),
                pltpu.make_async_copy(g_hbm.at[at], g_ref.at[at], local.at[1, g])]

    for g in range(ngr):
        for c in fetch(g):
            c.start()
    z_in = pltpu.make_async_copy(z_hbm, z_ref, local.at[2, 0])
    z_in.start()
    enter(axis, me, n)

    part = {None: slice(None), 0: pl.ds(0, half), 1: pl.ds(half, half)}

    def a_copies(g):
        seqs = pl.ds(pl.multiple_of(g * tb, tb), tb)
        src = lambda c, p=None: a_ref.at[c, part[p], seqs]
        dst = lambda d, p=None: ag_ref.at[d, part[p], seqs]
        tr = lambda t: tr_ref.at[t, :, seqs]
        plan = [(src(across, 0), tr(0), right), (src(across, 1), tr(1), left), (src(up), dst(me), right),
                (src(down), dst(me), left), (src(chip), dst(me), other),
                (tr(0), dst(left, 0), right), (tr(1), dst(right, 1), left),
                (dst(left), dst(left), other), (dst(right), dst(right), other),
                (dst(far, 0), dst(far, 0), other), (dst(far, 1), dst(far, 1), other)]
        return lambda k: remote(axis, (asend.at[g, k], arecv.at[g, k]), *plan[k])

    def b_first(g):
        seqs = pl.ds(pl.multiple_of(g * tb, tb), tb)
        return Gather(axis, me, n, lambda k: (bsend.at[g, k], brecv.at[g, k]), b_ref.at[0, :, seqs],
                      lambda d, p=None: bg_all.at[0, d, part[p], seqs])

    def b_rest(t):
        return Gather(axis, me, n, lambda k: (bsend.at[ngr - 1 + t, k], brecv.at[ngr - 1 + t, k]), b_ref.at[t],
                      lambda d, p=None: bg_all.at[t, d] if p is None else bg_all.at[t, d, part[p]])

    src = lax.broadcasted_iota(jnp.int32, (res, chips * jb), 0)
    dst = lax.broadcasted_iota(jnp.int32, (res, chips * jb), 1)
    hj = jb // 2
    place = ((dst % hj < rows) & (src == (dst // hj) * rows + dst % hj)).astype(BF16)

    wout, tin, opm = (flip(r[...]) for r in (wout_ref, tin_ref, opm_ref))
    gate_bias = column(bg_ref[...])
    column_attention(axis, n, heads, hd, scale, qsum_ref, cnt_ref, kv_ref, m_ref, o_ref,
                     l_ref, qp_ref, qb_ref, st_ref, sp_ref, csend, crecv)

    def group(g, _):
        seqs = pl.ds(pl.multiple_of(g * tb, tb), tb)
        for c in fetch(g):
            c.wait()
        o = jnp.concatenate([o_ref[...].reshape(ht, res)] * us, axis=1)
        for j in range(per):
            gr = g * per + j
            gated = (sigmoid(g_ref[gr].astype(F32) + gate_bias) * o).astype(BF16)
            e2 = (e1_ref[gr].astype(F32) + dot(wout, gated)).astype(BF16).astype(F32)
            hid = jnp.maximum(dot(tin, norm_rows(e2)), 0.0).astype(BF16)
            e3 = (e2 + dot(tout_ref[...], hid)).astype(BF16)
            ab = dot(opm, norm_rows(e3.astype(F32))).astype(BF16).astype(F32) * mask_row(m_ref, gr * us, us)
            for u in range(us):
                cols = slice(u * res, (u + 1) * res)
                e3_ref[gr * us + u] = e3[:, cols]
                buf_ref[:, j * us + u, :] = ab[:, cols]
        moved = dot(buf_ref[0:odim].astype(BF16).reshape(odim * tb, res), place).astype(BF16)
        for c in range(chips):
            a_ref[c, :, seqs, :] = moved[:, c * jb:(c + 1) * jb].reshape(odim, tb, jb)
        for t in range(nb):
            blk = buf_ref[odim:, :, t * jb:(t + 1) * jb].astype(BF16)
            b_ref[t, :, seqs, :] = blk
            bg_all[t, me, :, seqs, :] = blk
        ac = a_copies(g)
        for k in range(5):
            ac(k).start()
        b_first(g).open()
        ag_ref[me, :, seqs, :] = a_ref[chip, :, seqs, :]
        return 0

    lax.fori_loop(0, ngr, group, 0)
    e3_out = pltpu.make_async_copy(e3_ref, e3_hbm, local.at[2, 1])
    e3_out.start()

    def pass_on(g, _):
        ac = a_copies(g)
        for wait, start in ((0, 5), (1, 6), (2, 7), (3, 8)):
            ac(wait).wait_recv()
            ac(start).start()
        b_first(g).hand_on()
        return 0

    lax.fori_loop(0, ngr, pass_on, 0)
    b_rest(1).open()

    def finish_a(g, _):
        ac = a_copies(g)
        for wait, start in ((5, 9), (6, 10)):
            ac(wait).wait_recv()
            ac(start).start()
        for k in (4, 7, 8, 9, 10):
            ac(k).wait_recv()
        for k in range(11):
            ac(k).wait_send()
        return 0

    lax.fori_loop(0, ngr, finish_a, 0)
    wf_ref[...] = w_ref[...].astype(F32)
    for d in range(odim):
        wp_ref[:, d * odim:(d + 1) * odim] = jnp.transpose(wf_ref[:, d, :]).astype(BF16)
    pick = (lax.broadcasted_iota(jnp.int32, (rows, jb), 1) ==
            lax.broadcasted_iota(jnp.int32, (rows, jb), 0) + core * hj).astype(BF16)
    for c in range(odim):
        at_ref[:, c, :] = dot_t(pick, ag_ref[:, c].reshape(n * ns, jb))

    def finish_b(g, _):
        b_first(g).close()
        return 0

    lax.fori_loop(0, ngr, finish_b, 0)
    z_in.wait()
    steps = rows // ib

    def done(t):
        at = pl.ds(t * jb, jb)
        return pltpu.make_async_copy(z_ref.at[:, at], out_hbm.at[:, at], local.at[3, t])

    def body(k, _):
        t = k // steps
        base = lax.rem(k, steps) * ib
        cols = pl.ds(pl.multiple_of(t * jb, jb), jb)

        for later in range(1, nb):
            @pl.when(k == (later - 1) * steps + steps // 2)
            def _():
                b_rest(later).hand_on()
                if later + 1 < nb:
                    b_rest(later + 1).open()

            @pl.when(k == later * steps)
            def _():
                b_rest(later).close()
                done(later - 1).start()

        a = at_ref[pl.ds(base, ib)].reshape(ib * odim, n * ns).astype(BF16)
        for q in range(odim // 2):
            rhs = jnp.concatenate([bg_all[t, :, 2 * q].reshape(n * ns, jb), bg_all[t, :, 2 * q + 1].reshape(n * ns, jb)], axis=1)
            pr = dot(a, rhs)
            hi = pr.astype(BF16)
            lo = (pr - hi.astype(F32)).astype(BF16)
            for val, ref in ((hi, hi_ref), (lo, lo_ref)):
                for i in range(ib):
                    for h in range(2):
                        ref[i // 2, (2 * q + h) * odim:(2 * q + h + 1) * odim, (i % 2) * jb:(i % 2 + 1) * jb] = \
                            val[i * odim:(i + 1) * odim, h * jb:(h + 1) * jb]
        for ip in range(ib // 2):
            zt = dot(wp_ref[...], hi_ref[ip]) + dot(wp_ref[...], lo_ref[ip])
            for h in range(2):
                i = base + 2 * ip + h
                upd = jnp.transpose(zt[:, h * jb:(h + 1) * jb] * ninv_ref[i, :, cols])
                z_ref[i, cols, :] = (z_ref[i, cols, :].astype(F32) + upd + bo_ref[...].astype(F32)).astype(BF16)
        return 0

    lax.fori_loop(0, nb * steps, body, 0)
    done(nb - 1).start()
    for t in range(nb):
        done(t).wait()
    e3_out.wait()


def solution(mesh):
    row_spec = P(('batch', 'seq'))
    rep_spec = P()
    n_seq = mesh.shape['seq']

    def local_block(msa, mask, pair, w_pair_bias, w_row_in, b_row_gate, w_row_out, w_col_in, b_col_gate, w_col_out,
                    w_trans_in, w_trans_out, w_opm_in, w_opm_out, b_opm_out):
        ns, res, ch = msa.shape
        rows = pair.shape[0]
        pd = pair.shape[-1]
        heads = w_pair_bias.shape[1]
        ht = w_row_out.shape[0]
        hd = ht // heads
        odim = w_opm_out.shape[0]
        scale = hd ** -0.5
        params = functools.partial(pltpu.CompilerParams, vmem_limit_bytes=VMEM_LIMIT)

        vm = pl.BlockSpec(memory_space=pltpu.VMEM)
        hbm = pl.BlockSpec(memory_space=pl.ANY)
        dma = pltpu.SemaphoreType.DMA
        tall = 16
        nblk = rows // tall
        packed, _, ninv, counts = pl.pallas_call(
            functools.partial(bias_kernel, 'seq', n_seq),
            in_specs=[hbm, vm, vm],
            out_specs=[vm] * 4,
            out_shape=[jax.ShapeDtypeStruct((n_seq, nblk, heads, tall, res), BF16), jax.ShapeDtypeStruct((n_seq, ns, res), BF16),
                       jax.ShapeDtypeStruct((rows, 1, res), F32), jax.ShapeDtypeStruct((1, res), F32)],
            scratch_shapes=[pltpu.VMEM((rows, res, pd), BF16), pltpu.VMEM((heads, tall, res), F32), dma((nblk,)),
                            dma((nblk + 1, 9)), dma((nblk + 1, 9))],
            compiler_params=params(collective_id=1, has_side_effects=True),
            name='pair_bias',
        )(pair, w_pair_bias.T, mask)

        us = SEQS
        ng, wide = ns // us, us * res
        ncol = w_col_in.shape[1]

        full = lambda *shape: pl.BlockSpec(shape, lambda *g: (0,) * len(shape))
        group = lambda k, r: pl.BlockSpec((k, r, wide), lambda s: (s, 0, 0))
        e1, gate, kv, qsum = pl.pallas_call(
            functools.partial(row_kernel, heads, hd, scale),
            grid=(ng,),
            in_specs=[pl.BlockSpec((us, ch, res), lambda s: (s, 0, 0)), full(ns, res),
                      full(n_seq, nblk, heads, tall, res), full(ch, 4 * ht), full(1, ht), full(ht, ch), full(ch, ncol)],
            out_specs=[group(1, ch), group(1, ht), group(1, 2 * hd), full(ht, res)],
            out_shape=[jax.ShapeDtypeStruct((ng, ch, wide), BF16), jax.ShapeDtypeStruct((ng, ht, wide), BF16),
                       jax.ShapeDtypeStruct((ng, 2 * hd, wide), BF16), jax.ShapeDtypeStruct((ht, res), F32)],
            scratch_shapes=[pltpu.VMEM((us, 2 * GROUP * hd + 16, heads * res), BF16), pltpu.VMEM((heads // GROUP, wide, 2 * GROUP * hd + 16), BF16),
                            pltpu.VMEM((ht, wide), BF16), pltpu.VMEM((ht, wide), F32),
                            pltpu.VMEM((heads // GROUP, res, GROUP * res), F32), pltpu.VMEM((ch, wide), BF16), pltpu.VMEM((4 * ht, ch), BF16),
                            pltpu.VMEM((ch, ht), BF16), pltpu.VMEM((ncol, ch), BF16), pltpu.VMEM((ht, 1), F32), pltpu.SMEM((1,), F32)],
            compiler_params=params(dimension_semantics=('arbitrary',)),
            name='row_attention',
        )(jnp.transpose(msa, (0, 2, 1)), mask, packed, w_row_in, b_row_gate.reshape(1, ht), w_row_out, w_col_in)

        tb, jb, ib = 16, 128, 8
        chips = n_seq // 2
        nb = res // jb
        e3, pair_out = pl.pallas_call(
            functools.partial(tail_kernel, 'seq', n_seq, heads, hd, scale),
            in_specs=[vm] * 3 + [hbm] * 2 + [vm] * 6 + [hbm] + [vm] * 3,
            out_specs=[hbm, hbm],
            out_shape=[jax.ShapeDtypeStruct((ns, ch, res), BF16), jax.ShapeDtypeStruct((rows, res, pd), BF16)],
            scratch_shapes=[pltpu.VMEM((heads, hd, res), F32), pltpu.VMEM((ng, heads, wide), F32),
                            pltpu.VMEM((n_seq, ht // n_seq, res), F32), pltpu.VMEM((n_seq, ht // n_seq, res), F32),
                            pltpu.VMEM((heads, 16, res), F32), pltpu.VMEM((n_seq, 16, res), F32), dma((4, n_seq)), dma((4, n_seq)),
                            pltpu.VMEM((ng, ch, wide), BF16), pltpu.VMEM((ng, ht, wide), BF16), pltpu.VMEM((ns, ch, res), BF16),
                            pltpu.VMEM((rows, res, pd), BF16), pltpu.VMEM((2 * odim, tb, res), F32),
                            pltpu.VMEM((chips, odim, ns, jb), BF16), pltpu.VMEM((nb, odim, ns, jb), BF16),
                            pltpu.VMEM((n_seq, odim, ns, jb), BF16), pltpu.VMEM((2, odim // 2, ns, jb), BF16),
                            pltpu.VMEM((nb, n_seq, odim, ns, jb), BF16), pltpu.VMEM((rows, odim, n_seq * ns), F32),
                            pltpu.VMEM((ib // 2, odim * odim, 2 * jb), BF16), pltpu.VMEM((ib // 2, odim * odim, 2 * jb), BF16),
                            pltpu.VMEM((pd, odim * odim), BF16), pltpu.VMEM((odim, odim, pd), F32),
                            dma((4, max(4, ns // tb))), dma((ns // tb, 11)), dma((ns // tb, 11)),
                            dma((ns // tb + nb - 1, 9)), dma((ns // tb + nb - 1, 9))],
            compiler_params=params(collective_id=2, has_side_effects=True),
            name='tail_outer_product',
        )(qsum, counts, kv, e1, gate, mask, b_col_gate.reshape(1, ht), w_col_out, w_trans_in, w_trans_out.T, w_opm_in,
          pair, ninv, w_opm_out, b_opm_out.reshape(1, pd))
        return jnp.transpose(e3, (0, 2, 1)), pair_out

    return jax.shard_map(local_block, mesh=mesh, in_specs=(row_spec, row_spec, row_spec) + (rep_spec,) * 12,
                         out_specs=(row_spec, row_spec), check_vma=False)
```

```python
import functools
import math

import jax
import jax.numpy as jnp
from jax import lax
from jax.experimental import pallas as pl
from jax.experimental.pallas import tpu as pltpu
from jax.sharding import PartitionSpec as P

MASK_FILL = -1e9
LOG2E = math.log2(math.e)
F32 = jnp.float32
BF16 = jnp.bfloat16
VMEM_LIMIT = 62 * 1024 * 1024
MESH = pl.DeviceIdType.MESH
SEQS = 8
GROUP = 4


def norm_rows(x):
    c = x - jnp.mean(x, axis=0, keepdims=True)
    var = jnp.mean(c * c, axis=0, keepdims=True)
    return (c * lax.rsqrt(var + 1e-5)).astype(BF16)


def dot(a, b):
    return jnp.dot(a, b, preferred_element_type=F32)


def dot_t(a, b):
    return lax.dot_general(a, b, (((1,), (1,)), ((), ())), preferred_element_type=F32)


def sigmoid(x):
    return 0.5 * jnp.tanh(0.5 * x) + 0.5


def wide_max(x):
    return jnp.max(jnp.max(x, axis=0, keepdims=True), axis=1, keepdims=True)[0, 0]


def enter(axis, me, n):
    barrier = pltpu.get_barrier_semaphore()
    for t in range(1, n):
        pl.semaphore_signal(barrier, inc=1, device_id={axis: lax.rem(me + t, n)}, device_id_type=MESH)
    pl.semaphore_wait(barrier, n - 1)


def neighbours(me, n):
    return lax.rem(me + 2, n), lax.rem(me + n - 2, n), lax.rem(me + 4, n), me + 1 - 2 * lax.rem(me, 2)


def remote(axis, sems, src, dst, to):
    return pltpu.make_async_remote_copy(src_ref=src, dst_ref=dst, send_sem=sems[0], recv_sem=sems[1],
                                        device_id={axis: to}, device_id_type=MESH)


class Gather:
    def __init__(self, axis, me, n, sems, own, view):
        right, left, far, other = neighbours(me, n)
        plan = [(own, view(me), right), (own, view(me), left), (own, view(me), other),
                (view(left, 0), view(left, 0), right), (view(right, 1), view(right, 1), left),
                (view(left), view(left), other), (view(right), view(right), other),
                (view(far, 0), view(far, 0), other), (view(far, 1), view(far, 1), other)]
        self.copy = lambda k: remote(axis, sems(k), *plan[k])

    def after(self, waits, starts):
        for k in waits:
            self.copy(k).wait_recv()
        for k in starts:
            self.copy(k).start()

    def open(self):
        self.after((), (0, 1, 2))

    def hand_on(self):
        self.after((0,), (3, 5))
        self.after((1,), (4, 6))

    def close(self):
        self.after((3,), (7,))
        self.after((4,), (8,))
        self.after((2, 5, 6, 7, 8), ())
        for k in range(9):
            self.copy(k).wait_send()


def identity(size):
    return (lax.broadcasted_iota(jnp.int32, (size, size), 0) == lax.broadcasted_iota(jnp.int32, (size, size), 1)).astype(BF16)


def flip(x):
    return jnp.transpose(x.astype(F32)).astype(BF16)


def column(row):
    k = row.shape[1]
    on = lax.broadcasted_iota(jnp.int32, (k, k), 0) == lax.broadcasted_iota(jnp.int32, (k, k), 1)
    return jnp.sum(jnp.where(on, jnp.broadcast_to(row.astype(F32), (k, k)), 0.0), axis=1, keepdims=True)


def mask_row(m_ref, first, count):
    return jnp.concatenate([m_ref[pl.ds(first + u, 1), :] for u in range(count)], axis=1).astype(F32)


def bias_kernel(axis, n, z_hbm, w_ref, m_ref, out_ref, mask_ref, ninv_ref, cnt_ref, z_ref, blk_ref, local, send_sem, recv_sem):
    rows, res, pd = z_ref.shape
    heads = w_ref.shape[0]
    nblk, tall = out_ref.shape[1], out_ref.shape[3]
    ns = m_ref.shape[0]
    step = 4
    me = lax.axis_index(axis)

    def fetch(ib):
        at = pl.ds(ib * tall, tall)
        return pltpu.make_async_copy(z_hbm.at[at], z_ref.at[at], local.at[ib])

    for ib in range(nblk):
        fetch(ib).start()
    mask_ref[me] = m_ref[...].astype(BF16)
    enter(axis, me, n)
    hh, hs = heads // 2, ns // 2
    sems = lambda t: lambda k: (send_sem.at[t, k], recv_sem.at[t, k])
    mask_ring = Gather(axis, me, n, sems(nblk), mask_ref.at[me],
                       lambda d, p=None: mask_ref.at[d] if p is None else mask_ref.at[d, pl.ds(p * hs, hs)])

    def ring(ib):
        return Gather(axis, me, n, sems(ib), out_ref.at[me, ib],
                      lambda d, p=None: out_ref.at[d, ib] if p is None else out_ref.at[d, ib, pl.ds(p * hh, hh)])

    mask_ring.open()
    eye = identity(pd)

    def block(ib, _):
        fetch(ib).wait()
        for t in range(tall // step):
            zt = dot_t(eye, z_ref[pl.ds(ib * tall + t * step, step)].reshape(step * res, pd))
            b = dot(w_ref[...], norm_rows(zt))
            for u in range(step):
                blk_ref[:, t * step + u, :] = b[:, u * res:(u + 1) * res]
        out_ref[me, ib] = blk_ref[...].astype(BF16)
        ring(ib).open()
        return 0

    lax.fori_loop(0, nblk, block, 0)
    mask_ring.hand_on()
    for ib in range(nblk):
        ring(ib).hand_on()
    mask_ring.close()
    mask = mask_ref[...].reshape(n * ns, res)
    pick = (lax.broadcasted_iota(jnp.int32, (rows, res), 1) ==
            lax.broadcasted_iota(jnp.int32, (rows, res), 0) + me * rows).astype(BF16)
    pairs = dot(dot_t(pick, mask).astype(BF16), mask)
    ninv = 1.0 / (pairs + 1e-3)
    for i in range(rows):
        ninv_ref[i] = ninv[i:i + 1]
    cnt_ref[...] = dot(jnp.ones((8, n * ns), BF16), mask)[0:1]
    for ib in range(nblk):
        ring(ib).close()


def row_kernel(heads, hd, scale, e_ref, m_ref, packed_ref, win_ref, bg_ref, wout_ref, cin_ref,
               e1_ref, g_ref, kv_ref, qsum_ref,
               rhs_ref, kaug_ref, v_ref, att_ref, bias_ref, xn_ref, wt_ref, ot_ref, ct_ref, gb_ref, top_ref):
    us, ch, res = e_ref.shape
    ht = heads * hd
    wide = us * res
    step = pl.program_id(0)

    @pl.when(step == 0)
    def _():
        rows = lax.broadcasted_iota(jnp.int32, rhs_ref.shape, 1)
        rhs_ref[...] = jnp.where(rows == 2 * GROUP * hd, 1.0, 0.0).astype(BF16)
        qsum_ref[...] = jnp.zeros_like(qsum_ref)
        wt_ref[...] = flip(win_ref[...])
        ot_ref[...] = flip(wout_ref[...])
        ct = flip(cin_ref[...])
        r = lax.broadcasted_iota(jnp.int32, (ht, ht), 0)
        turn = (lax.broadcasted_iota(jnp.int32, (ht, ht), 1) == lax.rem(r, heads) * hd + r // heads).astype(BF16)
        ct_ref[...] = jnp.concatenate([dot(turn, ct[:ht]).astype(BF16), ct[ht:]], axis=0)
        gb_ref[...] = column(bg_ref[...])
        for h in range(heads):
            one = jnp.concatenate([packed_ref[d, t, h] for d in range(packed_ref.shape[0])
                                   for t in range(packed_ref.shape[1])], axis=0)
            bias_ref[h // GROUP, :, (h % GROUP) * res:(h % GROUP + 1) * res] = jnp.transpose(one.astype(F32)) * LOG2E
        top = jnp.abs(bias_ref[0])
        for gr in range(1, heads // GROUP):
            top = jnp.maximum(top, jnp.abs(bias_ref[gr]))
        top_ref[0] = wide_max(top)

    def source():
        return jnp.concatenate([e_ref[u] for u in range(us)], axis=1).astype(F32)

    def project(n):
        return dot(wt_ref[n * ht:(n + 1) * ht], xn_ref[...]).astype(BF16)

    xn_ref[...] = norm_rows(source())
    keep = mask_row(m_ref, step * us, us)
    qs = project(0).astype(F32) * (scale * LOG2E)
    k = project(1)
    v = project(2).astype(F32)
    per_head = (lax.broadcasted_iota(jnp.int32, (heads, ht), 1) // hd ==
                lax.broadcasted_iota(jnp.int32, (heads, ht), 0)).astype(BF16)
    q_top = wide_max(dot(per_head, (qs * qs).astype(BF16)))
    k_top = wide_max(dot(per_head, k * k))
    small = (q_top * k_top < 880.0) & (top_ref[0] < 30.0) & (wide_max(jnp.abs(v)) < 1e15)

    gw = GROUP * hd
    row_head = (lax.broadcasted_iota(jnp.int32, (ht, wide), 0) // hd) % GROUP
    hi = qs.astype(BF16).astype(F32)
    for n, part in enumerate((hi, qs - hi)):
        for r in range(GROUP):
            only = jnp.where(row_head == r, part, 0.0).astype(BF16)
            for u in range(us):
                for h in range(r, heads, GROUP):
                    rhs_ref[u, gw * n:gw * (n + 1), h * res:(h + 1) * res] = \
                        only[gw * (h // GROUP):gw * (h // GROUP + 1), u * res:(u + 1) * res]
    pen = jnp.where(lax.broadcasted_iota(jnp.int32, (16, wide), 0) == 0,
                    jnp.broadcast_to(jnp.where(keep > 0, 0.0, -1e30), (16, wide)), 0.0)
    for gr in range(heads // GROUP):
        kp = k[gw * gr:gw * (gr + 1)]
        kaug_ref[gr] = jnp.transpose(jnp.concatenate([kp, kp, pen.astype(BF16)], axis=0))
    v_ref[...] = v.astype(BF16)

    def attend(cols, gr, rows, lanes, at_row, shifted):
        s = dot(kaug_ref[gr, cols], lanes) + bias_ref[gr]
        p = jnp.exp2(s - jnp.max(s, axis=0, keepdims=True)) if shifted else jnp.exp2(s)
        o = dot(jnp.concatenate([v_ref[rows, cols], jnp.ones((16, res), BF16)], axis=0), p.astype(BF16))
        den = o[gw:gw + 1]
        for r in range(GROUP):
            att_ref[at_row(r), cols] = o[hd * r:hd * (r + 1), r * res:(r + 1) * res] / den[:, r * res:(r + 1) * res]

    @pl.when(small)
    def _():
        for u in range(us):
            cols = slice(u * res, (u + 1) * res)
            for gr in range(heads // GROUP):
                attend(cols, gr, slice(gw * gr, gw * (gr + 1)), rhs_ref[u, :, gr * GROUP * res:(gr + 1) * GROUP * res],
                       lambda r: slice(gw * gr + hd * r, gw * gr + hd * (r + 1)), False)
            some = jnp.max(keep[:, cols], axis=1, keepdims=True) > 0
            flat = jnp.mean(v[:, cols], axis=1, keepdims=True)
            att_ref[:, cols] = jnp.where(some, att_ref[:, cols], flat)

    @pl.when(jnp.logical_not(small))
    def _():
        def one(t, _):
            u, gr = t // (heads // GROUP), t % (heads // GROUP)
            cols = pl.ds(pl.multiple_of(u * res, res), res)
            attend(cols, gr, pl.ds(pl.multiple_of(gw * gr, gw), gw),
                   rhs_ref[u, :, pl.ds(pl.multiple_of(gr * GROUP * res, GROUP * res), GROUP * res)],
                   lambda r: pl.ds(pl.multiple_of(gw * gr + hd * r, hd), hd), True)
            return 0

        lax.fori_loop(0, us * (heads // GROUP), one, 0)

    gated = (sigmoid(project(3).astype(F32) + gb_ref[...]) * att_ref[...]).astype(BF16)
    e1 = (source() + dot(ot_ref[...], gated)).astype(BF16)
    e1_ref[0] = e1
    col = dot(ct_ref[...], norm_rows(e1.astype(F32))).astype(BF16)
    part = col[:ht].astype(F32) * keep
    tot = part[:, :res]
    for u in range(1, us):
        tot = tot + part[:, u * res:(u + 1) * res]
    qsum_ref[...] += tot
    g_ref[0] = col[ht:2 * ht]
    kv_ref[0] = col[2 * ht:]


def exchange(axis, me, n, srcs, dst, send_sem, recv_sem):
    copies = []
    for t in range(1, n):
        peer = lax.rem(me + t, n)
        copy = pltpu.make_async_remote_copy(src_ref=srcs(peer), dst_ref=dst.at[me], send_sem=send_sem.at[t],
                                            recv_sem=recv_sem.at[t], device_id={axis: peer}, device_id_type=MESH)
        copy.start()
        copies.append(copy)
    return copies


def column_attention(axis, n, heads, hd, scale, qsum_ref, cnt_ref, kv_ref, m_ref, o_ref,
                     l_ref, qp_ref, qb_ref, st_ref, sp_ref, send_sem, recv_sem):
    ng, _, wide = kv_ref.shape
    res = qsum_ref.shape[1]
    us = wide // res
    ht = heads * hd
    me = lax.axis_index(axis)
    blk = ht // n
    mine = pl.ds(pl.multiple_of(me * blk, blk), blk)
    copies = exchange(axis, me, n, lambda p: qsum_ref.at[pl.ds(pl.multiple_of(p * blk, blk), blk)], qp_ref,
                      send_sem.at[0], recv_sem.at[0])
    qp_ref[me] = qsum_ref[mine]
    for c in copies:
        c.wait()
    tot = qp_ref[0]
    for t in range(1, n):
        tot = tot + qp_ref[t]
    qb_ref[me] = (tot / (cnt_ref[...] + 1e-10)).astype(BF16).astype(F32)
    copies = exchange(axis, me, n, lambda p: qb_ref.at[me], qb_ref, send_sem.at[1], recv_sem.at[1])
    for c in copies:
        c.wait()
    qbar = qb_ref[...].reshape(ht, res)

    def logits(gr, top):
        for u in range(us):
            cols = slice(u * res, (u + 1) * res)
            kv = kv_ref[gr, :, cols].astype(F32)
            acc = qbar[0:heads] * kv[0:1]
            for d in range(1, hd):
                acc = acc + qbar[d * heads:(d + 1) * heads] * kv[d:d + 1]
            acc = jnp.where(m_ref[pl.ds(gr * us + u, 1), :] > 0, acc * scale, MASK_FILL)
            l_ref[gr, :, cols] = acc
            top = jnp.maximum(top, acc)
        return top

    top = lax.fori_loop(0, ng, logits, jnp.full((heads, res), -3e38, F32))

    def sums(gr, carry):
        for u in range(us):
            cols = slice(u * res, (u + 1) * res)
            w = jnp.exp(l_ref[gr, :, cols] - top)
            kv = kv_ref[gr, :, cols].astype(F32)
            carry = (carry[0] + w,) + tuple(carry[1 + d] + w * kv[hd + d:hd + d + 1] for d in range(hd))
        return carry

    zero = jnp.zeros((heads, res), F32)
    tot = lax.fori_loop(0, ng, sums, (zero,) * (hd + 1))
    for d in range(hd):
        st_ref[:, d, :] = tot[1 + d]
    st_ref[:, hd, :] = tot[0]
    st_ref[:, hd + 1, :] = top
    for d in range(hd + 2, st_ref.shape[1]):
        st_ref[:, d, :] = zero
    copies = exchange(axis, me, n, lambda p: st_ref.at[p], sp_ref, send_sem.at[2], recv_sem.at[2])
    sp_ref[me] = st_ref[me]
    for c in copies:
        c.wait()
    best = sp_ref[0, hd + 1:hd + 2]
    for t in range(1, n):
        best = jnp.maximum(best, sp_ref[t, hd + 1:hd + 2])
    num = jnp.zeros((hd, res), F32)
    den = jnp.zeros((1, res), F32)
    for t in range(n):
        fac = jnp.exp(sp_ref[t, hd + 1:hd + 2] - best)
        num = num + sp_ref[t, 0:hd] * fac
        den = den + sp_ref[t, hd:hd + 1] * fac
    o_ref[me] = num / den
    copies = exchange(axis, me, n, lambda p: o_ref.at[me], o_ref, send_sem.at[3], recv_sem.at[3])
    for c in copies:
        c.wait()


def tail_kernel(axis, n, heads, hd, scale, qsum_ref, cnt_ref, kv_ref, e1_hbm, g_hbm, m_ref, bg_ref, wout_ref, tin_ref, tout_ref, opm_ref,
                z_hbm, ninv_ref, w_ref, bo_ref, e3_hbm, out_hbm,
                o_ref, l_ref, qp_ref, qb_ref, st_ref, sp_ref, csend, crecv, e1_ref, g_ref, e3_ref, z_ref, buf_ref, a_ref, b_ref, ag_ref, tr_ref, bg_all, at_ref, hi_ref, lo_ref,
                wp_ref, wf_ref, place_ref, local, asend, arecv, bsend, brecv):
    rows, res, pd = z_ref.shape
    nb, odim, ns, jb = b_ref.shape
    chips = a_ref.shape[0]
    ht = heads * hd
    wide = e1_ref.shape[2]
    us = wide // res
    tb = buf_ref.shape[1]
    ngr = ns // tb
    per = tb // us
    ib = 2 * hi_ref.shape[0]
    half = odim // 2
    me = lax.axis_index(axis)
    chip, core = me // 2, lax.rem(me, 2)
    right, left, far, other = neighbours(me, n)
    up, down, across = lax.rem(chip + 1, chips), lax.rem(chip + chips - 1, chips), lax.rem(chip + 2, chips)

    def fetch(g):
        at = pl.ds(g * per, per)
        return [pltpu.make_async_copy(e1_hbm.at[at], e1_ref.at[at], local.at[0, g]),
                pltpu.make_async_copy(g_hbm.at[at], g_ref.at[at], local.at[1, g])]

    for g in range(ngr):
        for c in fetch(g):
            c.start()
    z_in = pltpu.make_async_copy(z_hbm, z_ref, local.at[2, 0])
    z_in.start()
    enter(axis, me, n)

    part = {None: slice(None), 0: pl.ds(0, half), 1: pl.ds(half, half)}
    quad = a_ref.shape[1]
    apart = {None: slice(None), 0: pl.ds(0, quad // 2), 1: pl.ds(quad // 2, quad // 2)}

    def a_copies(g):
        seqs = pl.ds(pl.multiple_of(g * tb, tb), tb)
        src = lambda c, p=None: a_ref.at[c, apart[p], seqs]
        dst = lambda d, p=None: ag_ref.at[d, apart[p], seqs]
        tr = lambda t: tr_ref.at[t, :, seqs]
        plan = [(src(across, 0), tr(0), right), (src(across, 1), tr(1), left), (src(up), dst(me), right),
                (src(down), dst(me), left), (src(chip), dst(me), other),
                (tr(0), dst(left, 0), right), (tr(1), dst(right, 1), left),
                (dst(left), dst(left), other), (dst(right), dst(right), other),
                (dst(far, 0), dst(far, 0), other), (dst(far, 1), dst(far, 1), other)]
        return lambda k: remote(axis, (asend.at[g, k], arecv.at[g, k]), *plan[k])

    def b_first(g):
        seqs = pl.ds(pl.multiple_of(g * tb, tb), tb)
        return Gather(axis, me, n, lambda k: (bsend.at[g, k], brecv.at[g, k]), b_ref.at[0, :, seqs],
                      lambda d, p=None: bg_all.at[0, d, part[p], seqs])

    def b_rest(t):
        return Gather(axis, me, n, lambda k: (bsend.at[ngr - 1 + t, k], brecv.at[ngr - 1 + t, k]), b_ref.at[t],
                      lambda d, p=None: bg_all.at[t, d] if p is None else bg_all.at[t, d, part[p]])

    pack = odim // quad
    src = lax.broadcasted_iota(jnp.int32, (res, chips * res), 0)
    dst = lax.broadcasted_iota(jnp.int32, (res, chips * res), 1)
    for r in range(pack):
        where = (dst // res) * (2 * rows) + dst % res - r * 2 * rows
        ok = (dst % res >= r * 2 * rows) & (dst % res < (r + 1) * 2 * rows)
        place_ref[r] = (ok & (src == where)).astype(BF16)

    wout, tin, opm = (flip(r[...]) for r in (wout_ref, tin_ref, opm_ref))
    gate_bias = column(bg_ref[...])
    column_attention(axis, n, heads, hd, scale, qsum_ref, cnt_ref, kv_ref, m_ref, o_ref,
                     l_ref, qp_ref, qb_ref, st_ref, sp_ref, csend, crecv)

    def group(g, _):
        seqs = pl.ds(pl.multiple_of(g * tb, tb), tb)
        for c in fetch(g):
            c.wait()
        o = jnp.concatenate([o_ref[...].reshape(ht, res)] * us, axis=1)
        for j in range(per):
            gr = g * per + j
            gated = (sigmoid(g_ref[gr].astype(F32) + gate_bias) * o).astype(BF16)
            e2 = (e1_ref[gr].astype(F32) + dot(wout, gated)).astype(BF16).astype(F32)
            hid = jnp.maximum(dot(tin, norm_rows(e2)), 0.0).astype(BF16)
            e3 = (e2 + dot(tout_ref[...], hid)).astype(BF16)
            ab = dot(opm, norm_rows(e3.astype(F32))).astype(BF16).astype(F32) * mask_row(m_ref, gr * us, us)
            for u in range(us):
                cols = slice(u * res, (u + 1) * res)
                e3_ref[gr * us + u] = e3[:, cols]
                buf_ref[:, j * us + u, :] = ab[:, cols]
        moved = sum(dot(buf_ref[r * quad:(r + 1) * quad].astype(BF16).reshape(quad * tb, res), place_ref[r]) for r in range(pack))
        for c in range(chips):
            a_ref[c, :, seqs, :] = moved[:, c * res:(c + 1) * res].astype(BF16).reshape(quad, tb, res)
        for t in range(nb):
            blk = buf_ref[odim:, :, t * jb:(t + 1) * jb].astype(BF16)
            b_ref[t, :, seqs, :] = blk
            bg_all[t, me, :, seqs, :] = blk
        ac = a_copies(g)
        for k in range(5):
            ac(k).start()
        b_first(g).open()
        ag_ref[me, :, seqs, :] = a_ref[chip, :, seqs, :]
        return 0

    lax.fori_loop(0, ngr, group, 0)
    e3_out = pltpu.make_async_copy(e3_ref, e3_hbm, local.at[2, 1])
    e3_out.start()

    def pass_on(g, _):
        ac = a_copies(g)
        for wait, start in ((0, 5), (1, 6), (2, 7), (3, 8)):
            ac(wait).wait_recv()
            ac(start).start()
        b_first(g).hand_on()
        return 0

    lax.fori_loop(0, ngr, pass_on, 0)
    b_rest(1).open()

    def finish_a(g, _):
        ac = a_copies(g)
        for wait, start in ((5, 9), (6, 10)):
            ac(wait).wait_recv()
            ac(start).start()
        for k in (4, 7, 8, 9, 10):
            ac(k).wait_recv()
        for k in range(11):
            ac(k).wait_send()
        return 0

    lax.fori_loop(0, ngr, finish_a, 0)
    wf_ref[...] = w_ref[...].astype(F32)
    for d in range(odim):
        wp_ref[:, d * odim:(d + 1) * odim] = jnp.transpose(wf_ref[:, d, :]).astype(BF16)
    row = lax.broadcasted_iota(jnp.int32, (pack * rows, res), 0)
    pick = (lax.broadcasted_iota(jnp.int32, (pack * rows, res), 1) ==
            (row // rows) * (2 * rows) + row % rows + core * rows).astype(BF16)
    for q in range(quad):
        got = dot_t(pick, ag_ref[:, q].reshape(n * ns, res))
        for r in range(pack):
            at_ref[:, r * quad + q, :] = got[r * rows:(r + 1) * rows]

    def finish_b(g, _):
        b_first(g).close()
        return 0

    lax.fori_loop(0, ngr, finish_b, 0)
    z_in.wait()
    steps = rows // ib

    def done(t):
        at = pl.ds(t * jb, jb)
        return pltpu.make_async_copy(z_ref.at[:, at], out_hbm.at[:, at], local.at[3, t])

    def body(k, _):
        t = k // steps
        base = lax.rem(k, steps) * ib
        cols = pl.ds(pl.multiple_of(t * jb, jb), jb)

        for later in range(1, nb):
            @pl.when(k == (later - 1) * steps + steps // 2)
            def _():
                b_rest(later).hand_on()
                if later + 1 < nb:
                    b_rest(later + 1).open()

            @pl.when(k == later * steps)
            def _():
                b_rest(later).close()
                done(later - 1).start()

        a = at_ref[pl.ds(base, ib)].reshape(ib * odim, n * ns).astype(BF16)
        for q in range(odim // 2):
            rhs = jnp.concatenate([bg_all[t, :, 2 * q].reshape(n * ns, jb), bg_all[t, :, 2 * q + 1].reshape(n * ns, jb)], axis=1)
            pr = dot(a, rhs)
            hi = pr.astype(BF16)
            lo = (pr - hi.astype(F32)).astype(BF16)
            for val, ref in ((hi, hi_ref), (lo, lo_ref)):
                for i in range(ib):
                    for h in range(2):
                        ref[i // 2, (2 * q + h) * odim:(2 * q + h + 1) * odim, (i % 2) * jb:(i % 2 + 1) * jb] = \
                            val[i * odim:(i + 1) * odim, h * jb:(h + 1) * jb]
        for ip in range(ib // 2):
            zt = dot(wp_ref[...], hi_ref[ip]) + dot(wp_ref[...], lo_ref[ip])
            for h in range(2):
                i = base + 2 * ip + h
                upd = jnp.transpose(zt[:, h * jb:(h + 1) * jb] * ninv_ref[i, :, cols])
                z_ref[i, cols, :] = (z_ref[i, cols, :].astype(F32) + upd + bo_ref[...].astype(F32)).astype(BF16)
        return 0

    lax.fori_loop(0, nb * steps, body, 0)
    done(nb - 1).start()
    for t in range(nb):
        done(t).wait()
    e3_out.wait()


def solution(mesh):
    row_spec = P(('batch', 'seq'))
    rep_spec = P()
    n_seq = mesh.shape['seq']

    def local_block(msa, mask, pair, w_pair_bias, w_row_in, b_row_gate, w_row_out, w_col_in, b_col_gate, w_col_out,
                    w_trans_in, w_trans_out, w_opm_in, w_opm_out, b_opm_out):
        ns, res, ch = msa.shape
        rows = pair.shape[0]
        pd = pair.shape[-1]
        heads = w_pair_bias.shape[1]
        ht = w_row_out.shape[0]
        hd = ht // heads
        odim = w_opm_out.shape[0]
        scale = hd ** -0.5
        params = functools.partial(pltpu.CompilerParams, vmem_limit_bytes=VMEM_LIMIT)

        vm = pl.BlockSpec(memory_space=pltpu.VMEM)
        hbm = pl.BlockSpec(memory_space=pl.ANY)
        dma = pltpu.SemaphoreType.DMA
        tall = 16
        nblk = rows // tall
        packed, _, ninv, counts = pl.pallas_call(
            functools.partial(bias_kernel, 'seq', n_seq),
            in_specs=[hbm, vm, vm],
            out_specs=[vm] * 4,
            out_shape=[jax.ShapeDtypeStruct((n_seq, nblk, heads, tall, res), BF16), jax.ShapeDtypeStruct((n_seq, ns, res), BF16),
                       jax.ShapeDtypeStruct((rows, 1, res), F32), jax.ShapeDtypeStruct((1, res), F32)],
            scratch_shapes=[pltpu.VMEM((rows, res, pd), BF16), pltpu.VMEM((heads, tall, res), F32), dma((nblk,)),
                            dma((nblk + 1, 9)), dma((nblk + 1, 9))],
            compiler_params=params(collective_id=1, has_side_effects=True),
            name='pair_bias',
        )(pair, w_pair_bias.T, mask)

        us = SEQS
        ng, wide = ns // us, us * res
        ncol = w_col_in.shape[1]

        full = lambda *shape: pl.BlockSpec(shape, lambda *g: (0,) * len(shape))
        group = lambda k, r: pl.BlockSpec((k, r, wide), lambda s: (s, 0, 0))
        e1, gate, kv, qsum = pl.pallas_call(
            functools.partial(row_kernel, heads, hd, scale),
            grid=(ng,),
            in_specs=[pl.BlockSpec((us, ch, res), lambda s: (s, 0, 0)), full(ns, res),
                      full(n_seq, nblk, heads, tall, res), full(ch, 4 * ht), full(1, ht), full(ht, ch), full(ch, ncol)],
            out_specs=[group(1, ch), group(1, ht), group(1, 2 * hd), full(ht, res)],
            out_shape=[jax.ShapeDtypeStruct((ng, ch, wide), BF16), jax.ShapeDtypeStruct((ng, ht, wide), BF16),
                       jax.ShapeDtypeStruct((ng, 2 * hd, wide), BF16), jax.ShapeDtypeStruct((ht, res), F32)],
            scratch_shapes=[pltpu.VMEM((us, 2 * GROUP * hd + 16, heads * res), BF16), pltpu.VMEM((heads // GROUP, wide, 2 * GROUP * hd + 16), BF16),
                            pltpu.VMEM((ht, wide), BF16), pltpu.VMEM((ht, wide), F32),
                            pltpu.VMEM((heads // GROUP, res, GROUP * res), F32), pltpu.VMEM((ch, wide), BF16), pltpu.VMEM((4 * ht, ch), BF16),
                            pltpu.VMEM((ch, ht), BF16), pltpu.VMEM((ncol, ch), BF16), pltpu.VMEM((ht, 1), F32), pltpu.SMEM((1,), F32)],
            compiler_params=params(dimension_semantics=('arbitrary',)),
            name='row_attention',
        )(jnp.transpose(msa, (0, 2, 1)), mask, packed, w_row_in, b_row_gate.reshape(1, ht), w_row_out, w_col_in)

        tb, jb, ib = 16, 128, 8
        chips = n_seq // 2
        nb = res // jb
        quad = odim * 2 * rows // res
        e3, pair_out = pl.pallas_call(
            functools.partial(tail_kernel, 'seq', n_seq, heads, hd, scale),
            in_specs=[vm] * 3 + [hbm] * 2 + [vm] * 6 + [hbm] + [vm] * 3,
            out_specs=[hbm, hbm],
            out_shape=[jax.ShapeDtypeStruct((ns, ch, res), BF16), jax.ShapeDtypeStruct((rows, res, pd), BF16)],
            scratch_shapes=[pltpu.VMEM((heads, hd, res), F32), pltpu.VMEM((ng, heads, wide), F32),
                            pltpu.VMEM((n_seq, ht // n_seq, res), F32), pltpu.VMEM((n_seq, ht // n_seq, res), F32),
                            pltpu.VMEM((heads, 16, res), F32), pltpu.VMEM((n_seq, 16, res), F32), dma((4, n_seq)), dma((4, n_seq)),
                            pltpu.VMEM((ng, ch, wide), BF16), pltpu.VMEM((ng, ht, wide), BF16), pltpu.VMEM((ns, ch, res), BF16),
                            pltpu.VMEM((rows, res, pd), BF16), pltpu.VMEM((2 * odim, tb, res), F32),
                            pltpu.VMEM((chips, quad, ns, res), BF16), pltpu.VMEM((nb, odim, ns, jb), BF16),
                            pltpu.VMEM((n_seq, quad, ns, res), BF16), pltpu.VMEM((2, quad // 2, ns, res), BF16),
                            pltpu.VMEM((nb, n_seq, odim, ns, jb), BF16), pltpu.VMEM((rows, odim, n_seq * ns), F32),
                            pltpu.VMEM((ib // 2, odim * odim, 2 * jb), BF16), pltpu.VMEM((ib // 2, odim * odim, 2 * jb), BF16),
                            pltpu.VMEM((pd, odim * odim), BF16), pltpu.VMEM((odim, odim, pd), F32),
                            pltpu.VMEM((odim // quad, res, chips * res), BF16),
                            dma((4, max(4, ns // tb))), dma((ns // tb, 11)), dma((ns // tb, 11)),
                            dma((ns // tb + nb - 1, 9)), dma((ns // tb + nb - 1, 9))],
            compiler_params=params(collective_id=2, has_side_effects=True),
            name='tail_outer_product',
        )(qsum, counts, kv, e1, gate, mask, b_col_gate.reshape(1, ht), w_col_out, w_trans_in, w_trans_out.T, w_opm_in,
          pair, ninv, w_opm_out, b_opm_out.reshape(1, pd))
        return jnp.transpose(e3, (0, 2, 1)), pair_out

    return jax.shard_map(local_block, mesh=mesh, in_specs=(row_spec, row_spec, row_spec) + (rep_spec,) * 12,
                         out_specs=(row_spec, row_spec), check_vma=False)
```
